256 devices in a mesh: fsdp: 32 (over x_hi, z, core), tp: 8 (over x_lo, y).
Axes of the slice: x: 4 (x_hi: 2, x_lo: 2; x = x_hi * 2 + x_lo), y: 4, z: 8, core: 2. Of those that a mesh axis runs over, the one named last changes fastest.
Arguments:
- tokens: bfloat16 [4096, 3584], P('fsdp', 'tp'), may hold values from -6 to 6
- norm_gain: bfloat16 [3584], replicated, may hold values from 0.5 to 1.5
- gate_weight: bfloat16 [3584, 10240], P('fsdp', 'tp'), may hold values from -0.09375 to 0.09375
- up_weight: bfloat16 [3584, 10240], P('fsdp', 'tp'), may hold values from -0.09375 to 0.09375
- down_weight: bfloat16 [3584, 10240], P('fsdp', 'tp'), may hold values from -0.0625 to 0.0625
- probes: bfloat16 [2, 3584, 10240], P(None, 'fsdp', 'tp'), may hold values from -0.0625 to 0.0625
Outputs:
- layer_out: bfloat16 [4096, 3584], P('tp', 'fsdp')
- token_curv: float32 [4096], P('tp')
The draws below stay inside these ranges and needn't reach their ends.
All inputs are finite; a program needn't handle non-finite values.
Results may differ from the reference program's by a relative error of at most 0.014.
Values may be sent and summed in bfloat16 or wider, within the bound.
A program may use at most 64 MiB of HBM per device.

```python
import jax
import jax.numpy as jnp
from jax import lax

D = 3584
FF = 10240
PROBES = 2
TOKENS = 4096
N_TP = 8


def level_of(rng, dims, cuts, smallest, largest):
    def one(dim, parts):
        steps = jax.random.uniform(jax.random.fold_in(jax.random.fold_in(rng, 6), dim), (parts,), jnp.float32, smallest / len(cuts), largest / len(cuts))
        return jnp.repeat(jnp.exp(steps), dims[dim] // parts).reshape((-1,) + (1,) * (len(dims) - dim - 1))

    gain = one(*cuts[0])
    for cut in cuts[1:]:
        gain = gain * one(*cut)
    return gain


def bell_draw(own_key, dims, width, most, shards=(), dtype=jnp.bfloat16):
    factor_of = level_of(own_key, dims, shards, -0.22, 0.18) if shards else 1.0
    entries = jax.random.normal(own_key, dims, jnp.float32) * width * factor_of
    return jnp.minimum(jnp.maximum(entries, -most), most).astype(dtype)


def setup_inputs(seed: int = 0) -> dict:
    arg_keys = jax.random.split(jax.random.key(seed), 7)
    return {
        "tokens": bell_draw(arg_keys[0], (TOKENS, D), 1.0, 6.0, ((0, 32), (1, 8))),
        "norm_gain": jnp.clip(1.0 + 0.1 * jax.random.normal(arg_keys[1], (D,), jnp.float32), 0.5, 1.5).astype(jnp.bfloat16),
        "gate_weight": bell_draw(arg_keys[2], (D, FF), D ** -0.5, 0.09375, ((0, 32), (1, 8))),
        "up_weight": bell_draw(arg_keys[3], (D, FF), D ** -0.5, 0.09375, ((0, 32), (1, 8))),
        "down_weight": bell_draw(arg_keys[4], (D, FF), FF ** -0.5, 0.0625, ((0, 32), (1, 8))),
        "probes": bell_draw(arg_keys[5], (PROBES, D, FF), FF ** -0.5, 0.0625, ((1, 32), (2, 8))),
    }


epsilon = 1e-06

def reference(tokens, norm_gain, gate_weight, up_weight, down_weight, probes):
    widened = tokens.astype(jnp.float32)
    inverse_rms = lax.rsqrt(lax.optimization_barrier(jnp.mean(widened * widened, axis=1, keepdims=True)) + epsilon)
    normed = (widened * inverse_rms * norm_gain.astype(jnp.float32)).astype(jnp.bfloat16)
    gate_sum = jnp.dot(normed, gate_weight, preferred_element_type=jnp.float32)
    up_sum = jnp.dot(normed, up_weight, preferred_element_type=jnp.float32)
    hidden = (jax.nn.silu(gate_sum) * up_sum).astype(jnp.bfloat16)
    stacked = jnp.concatenate([down_weight[None], probes], axis=0)
    count = stacked.shape[0]
    block_width = FF // N_TP

    def add_block(block_index, running):
        offset = (block_index * block_width).astype(jnp.int32)
        columns = lax.dynamic_slice_in_dim(hidden, offset, block_width, 1)
        matrices = lax.dynamic_slice_in_dim(stacked, offset, block_width, 2)
        terms = [lax.dot_general(columns, matrices[which], (((1,), (1,)), ((), ())), preferred_element_type=jnp.float32).astype(jnp.bfloat16).astype(jnp.float32) for which in range(count)]
        return running + jnp.stack(terms)
    projected = lax.fori_loop(0, N_TP, add_block, jnp.zeros((count, TOKENS, D), jnp.float32))
    primal = projected[0]
    squashed = jax.nn.sigmoid(primal)
    slope = squashed * (1.0 - squashed)
    tangent_sq = lax.optimization_barrier(jnp.sum(projected[1:] * projected[1:], axis=0))
    token_curv = lax.optimization_barrier(jnp.sum(slope * tangent_sq, axis=1)) / (PROBES * D)
    return (primal.astype(jnp.bfloat16), token_curv)
```

```python
import jax
import jax.numpy as jnp
from jax import lax
from jax.experimental import pallas as pl
from jax.experimental.pallas import tpu as pltpu
from jax.sharding import PartitionSpec as P

MESH = pl.DeviceIdType.MESH
F32, BF16 = jnp.float32, jnp.bfloat16
D = 3584
PROBES = 2
EPS = 1e-06
KD = 112
FH = 640
TB = 128
DT = 448
XR = 224
NT = (((1,), (1,)), ((), ()))

SCRATCH = dict(
    xg=((8, 256, DT), BF16),
    xn=((8, 256, DT), BF16),
    w=((D, 2 * FH), BF16),
    acc=((256, 2 * FH), F32),
    h=((4096, FH), BF16),
    mx=((2, 3 * KD, FH), BF16),
    popp=((4, XR, 512), BF16),
    pr=((4, XR, 512), BF16),
    pl_=((4, XR, 512), BF16),
    ra=((4, XR, 256), BF16),
    rb=((4, XR, 256), BF16),
    rr=((4, XR, 512), BF16),
    rl=((4, XR, 512), BF16),
    s=((4, XR, 512), BF16),
    sf=((XR, 512), F32),
    ya=((XR, 256), BF16),
    yb=((XR, 256), BF16),
    yr=((XR, 512), BF16),
    yl=((XR, 512), BF16),
    q=((4, 4, KD, 512), BF16),
    qa=((2, KD, 512), BF16),
    qb=((2, KD, 512), BF16),
    qr=((4, KD, 512), BF16),
    ql=((4, KD, 512), BF16),
    tq=((4, KD, 512), BF16),
    tf=((KD, 512), F32),
    fa=((KD, 256), BF16),
    fb=((KD, 256), BF16),
    fr=((KD, 512), BF16),
    fl=((KD, 512), BF16),
    cvs=((3, 1, 512), F32),
    cvr=((10, 1, 512), F32),
)
SEMS = dict(
    tokx=(3,), toky=(2, 2, 2), w1=(2,), m1=(3,), wr=(2, 2, 4, 2), wd=(2, 8), hr=(2, 4, 2), hd=(8, 2),
    xa=(4, 2), xb=(4, 2, 2), qa=(2,), qb=(2, 2), ya=(2,), yb=(2, 2), fa=(2,), fb=(2, 2), cv=(10,),
)


class Refs:
    pass


def kernel(tok, gain, wg, wu, dn, pr, out, curv, *scratch):
    b, ss, rs = Refs(), Refs(), Refs()
    names = list(SCRATCH)
    for n, r in zip(names, scratch):
        setattr(b, n, r)
    rest = scratch[len(names):]
    for i, n in enumerate(SEMS):
        setattr(ss, n, rest[2 * i])
        setattr(rs, n, rest[2 * i + 1])
    loc = rest[2 * len(SEMS)]

    fi, ti = lax.axis_index("fsdp"), lax.axis_index("tp")
    X, z, c = fi // 16, lax.rem(fi // 2, 8), lax.rem(fi, 2)
    xl, y = ti // 4, lax.rem(ti, 4)
    x = X * 2 + xl

    def dev(x_=None, y_=None, z_=None, c_=None):
        x_ = x if x_ is None else x_
        y_ = y if y_ is None else y_
        z_ = z if z_ is None else z_
        c_ = c if c_ is None else c_
        return ((x_ // 2) * 16 + z_ * 2 + c_, lax.rem(x_, 2) * 4 + y_)

    xp, xm, xo = lax.rem(x + 1, 4), lax.rem(x + 3, 4), lax.rem(x + 2, 4)
    yp, ym = lax.rem(y + 1, 4), lax.rem(y + 3, 4)
    dxp, dxm, dxo = dev(x_=xp), dev(x_=xm), dev(x_=xo)
    dyp, dym = dev(y_=yp), dev(y_=ym)
    dz = (dev(z_=lax.rem(z + 1, 8)), dev(z_=lax.rem(z + 7, 8)))
    dc = dev(c_=1 - c)

    def copy(name, idx, src, dst, to):
        return pltpu.make_async_remote_copy(
            src_ref=src, dst_ref=dst, send_sem=getattr(ss, name).at[idx], recv_sem=getattr(rs, name).at[idx],
            device_id=to, device_id_type=MESH,
        )

    def send(name, idx, src, dst, to):
        copy(name, idx, src, dst, to).start()

    def got(name, idx, ref):
        copy(name, idx, ref, ref, dc).wait_recv()

    def sent(name, idx, ref):
        copy(name, idx, ref, ref, dc).wait_send()

    def cols(k):
        return pl.ds(pl.multiple_of(k * FH, 128), FH)

    def wrows(X_, z_, c_=None):
        c_ = c if c_ is None else c_
        return pl.ds(pl.multiple_of((X_ * 16 + z_ * 2 + c_) * KD, 16), KD)

    def wchunk(X_, z_, half):
        return b.w.at[wrows(X_, z_), pl.ds(half * FH, FH)]

    def hchunk(X_, z_):
        return b.h.at[pl.ds(pl.multiple_of((X_ * 16 + z_ * 2 + c) * TB, 128), TB), :]

    mine = [
        (tok, b.xg.at[ti, pl.ds(pl.multiple_of(X * TB, 128), TB), :]),
        (wg.at[:, cols(X)], wchunk(X, z, 0)),
        (wu.at[:, cols(X)], wchunk(X, z, 1)),
        (dn.at[:, cols(X)], b.mx.at[X, pl.ds(0, KD), :]),
        (pr.at[0, :, cols(X)], b.mx.at[X, pl.ds(KD, KD), :]),
        (pr.at[1, :, cols(X)], b.mx.at[X, pl.ds(2 * KD, KD), :]),
    ]
    own = [pltpu.make_async_copy(s_, d_, loc.at[i]) for i, (s_, d_) in enumerate(mine)]
    for o in own:
        o.start()

    barrier = pltpu.get_barrier_semaphore()
    zs = [lax.rem(z + r, 8) for r in range(8)]
    partners = [dxp, dxm, dxo, dyp, dym, dc] + [dev(z_=zs[r]) for r in range(1, 8)]
    for p in partners:
        pl.semaphore_signal(barrier, inc=1, device_id=p, device_id_type=MESH)
    pl.semaphore_wait(barrier, len(partners))

    for o in own:
        o.wait()

    def ring_start(sub, X_):
        for half in (0, 1):
            for d in (0, 1):
                send("wr", (d, sub, 0, half), wchunk(X_, z, half), wchunk(X_, z, half), dz[d])
        send("wd", (sub, 0), b.w.at[wrows(X_, z), :], b.w.at[wrows(X_, z), :], dc)

    ring_start(0, X)
    tx = b.xg.at[ti, pl.ds(pl.multiple_of(X * TB, 128), TB), :]
    for k, to in enumerate((dxp, dxm, dxo)):
        send("tokx", (k,), tok, tx, to)
    for half, src in enumerate((wg, wu)):
        send("w1", (half,), src.at[:, cols(1 - X)], wchunk(X, z, half), dxo)

    def m_send():
        for k, src in enumerate((dn, pr.at[0], pr.at[1])):
            send("m1", (k,), src.at[:, cols(1 - X)], b.mx.at[X, pl.ds(k * KD, KD), :], dxo)

    def zsrc(d, s_):
        return lax.rem(z + (8 - s_ if d == 0 else s_), 8)

    def ring_step(sub, X_, s_):
        for half in (0, 1):
            for d in (0, 1):
                if s_ == 4 and half != d:
                    continue
                ch = wchunk(X_, zsrc(d, s_), half)
                got("wr", (d, sub, s_ - 1, half), ch)
                if s_ < 3 or (s_ == 3 and half == d):
                    send("wr", (d, sub, s_, half), ch, ch, dz[d])
        for d in (0, 1):
            if s_ == 4 and d == 1:
                continue
            blk = b.w.at[wrows(X_, zsrc(d, s_)), :]
            send("wd", (sub, 8 - s_ if d == 0 else s_), blk, blk, dc)

    par = lax.rem(z, 2)

    def pair(i):
        f = 3 * i - 5 * (i // 2) - 2 * (i // 3)
        return lax.rem(z // 2 + f * (1 - par) + (4 - f) * par, 4)

    def other_core(sub, X_, s_):
        if s_ == 1:
            got("wd", (sub, 0), b.w.at[wrows(X_, z, 1 - c), :])
        for d in (0, 1):
            if s_ == 4 and d == 1:
                continue
            got("wd", (sub, 8 - s_ if d == 0 else s_), b.w.at[wrows(X_, zsrc(d, s_), 1 - c), :])

    def multiply(X_, s_):
        j = X_ * 4 + pair(s_ - 1)

        @pl.loop(0, 5)
        def _(n):
            cs = pl.ds(pl.multiple_of(n * 256, 256), 256)
            ks = pl.ds(pl.multiple_of(j * DT, 64), DT)
            b.acc[:, cs] += jnp.dot(b.xn[j], b.w[ks, cs], preferred_element_type=F32)

    def tokx_done():
        for k, sx in enumerate((xm, xp, xo)):
            got("tokx", (k,), b.xg.at[lax.rem(sx, 2) * 4 + y, pl.ds(pl.multiple_of((sx // 2) * TB, 128), TB), :])
        for k in (0, 1):
            blk = b.xg.at[k * 4 + y]
            send("toky", (0, k, 0), blk, blk, dyp)
            send("toky", (1, k, 0), blk, blk, dym)

    def toky_first():
        for d, sy, to in ((0, ym, dyp), (1, yp, dym)):
            for k in (0, 1):
                got("toky", (d, k, 0), b.xg.at[k * 4 + sy])
            blk = b.xg.at[d * 4 + sy]
            send("toky", (d, d, 1), blk, blk, to)

    def toky_last():
        for d in (0, 1):
            got("toky", (d, d, 1), b.xg.at[d * 4 + lax.rem(y + 2, 4)])

    def norm():
        @pl.loop(0, 8)
        def _(t):
            rows = pl.ds(pl.multiple_of(t * 32, 32), 32)
            total = jnp.zeros((32, 1), F32)
            for j in range(8):
                v = b.xg[j, rows, :].astype(F32)
                total += jnp.sum(v * v, axis=1, keepdims=True)
            inv = lax.rsqrt(total / D + EPS)
            for j in range(8):
                v = b.xg[j, rows, :].astype(F32)
                b.xn[j, rows, :] = (v * inv * gain[j : j + 1, :]).astype(BF16)

    b.acc[...] = jnp.zeros_like(b.acc)
    ring_step(0, X, 1)
    tokx_done()
    ring_step(0, X, 2)
    toky_first()
    ring_step(0, X, 3)
    for half in (0, 1):
        got("w1", (half,), wchunk(1 - X, z, half))
    ring_start(1, 1 - X)
    m_send()
    ring_step(0, X, 4)
    toky_last()
    norm()
    ring_step(1, 1 - X, 1)
    for s_ in (1, 2):
        other_core(0, X, s_)
        multiply(X, s_)
    ring_step(1, 1 - X, 2)
    for s_ in (3, 4):
        other_core(0, X, s_)
        multiply(X, s_)
    other_core(1, 1 - X, 1)
    multiply(1 - X, 1)
    ring_step(1, 1 - X, 3)
    other_core(1, 1 - X, 2)
    multiply(1 - X, 2)
    ring_step(1, 1 - X, 4)
    for s_ in (3, 4):
        other_core(1, 1 - X, s_)
        multiply(1 - X, s_)

    @pl.loop(0, 5)
    def _(n):
        cs = pl.ds(pl.multiple_of(n * 128, 128), 128)
        g = b.acc[:, cs]
        u = b.acc[:, pl.ds(pl.multiple_of(FH + n * 128, 128), 128)]
        hid = (g / (1.0 + jnp.exp(-g)) * u).astype(BF16)
        for k in (0, 1):
            b.h[pl.ds(pl.multiple_of((k * 16 + z * 2 + c) * TB, 128), TB), cs] = hid[k * TB : (k + 1) * TB]

    for k in (0, 1):
        for d in (0, 1):
            send("hr", (d, 0, k), hchunk(k, z), hchunk(k, z), dz[d])
        send("hd", (0, k), hchunk(k, z), hchunk(k, z), dc)
    for k in range(3):
        got("m1", (k,), b.mx.at[1 - X, pl.ds(k * KD, KD), :])

    def hother(k, z_):
        return b.h.at[pl.ds(pl.multiple_of((k * 16 + z_ * 2 + 1 - c) * TB, 128), TB), :]

    for k in (0, 1):
        got("hd", (0, k), hother(k, z))

    def h_step(s_):
        for k in (0, 1):
            for d in (0, 1):
                zz = lax.rem(z + (8 - s_ if d == 0 else s_), 8)
                r = 8 - s_ if d == 0 else s_
                ch = hchunk(k, zz)

                def take():
                    got("hr", (d, s_ - 1, k), ch)

                    @pl.when(s_ < (4 if k == d else 3))
                    def _():
                        send("hr", (d, s_, k), ch, ch, dz[d])

                    send("hd", (r, k), ch, ch, dc)

                if k == d:
                    take()
                else:
                    pl.when(s_ < 4)(take)
        for k in (0, 1):
            for d in (0, 1):
                zz = lax.rem(z + (8 - s_ if d == 0 else s_), 8)
                r = 8 - s_ if d == 0 else s_

                def take2():
                    got("hd", (r, k), hother(k, zz))

                if k == d:
                    take2()
                else:
                    pl.when(s_ < 4)(take2)

    def term(dx, k0, nk, m, lane, n):
        a = b.mx[dx // 2, k0 * KD : (k0 + nk) * KD, :]
        rows = pl.ds(pl.multiple_of(lax.rem(dx, 2) * 2048 + m * 512 + lane, 256), n)
        return lax.dot_general(a, b.h[rows, :], NT, preferred_element_type=F32)

    LO, HI = pl.ds(0, 256), pl.ds(256, 256)

    def rel_of(i):
        m = pair(i)
        return m, lax.rem(m - y + 4, 4)

    def part1(i):
        m, rel = rel_of(i)
        for k, lanes in enumerate((LO, HI)):
            b.popp[i, :, lanes] = term(xo, 1, 2, m, k * 256, 256).astype(BF16)
        send("xa", (i, 0), b.popp.at[i, :, LO], b.ra.at[i], dxp)
        send("xa", (i, 1), b.popp.at[i, :, HI], b.rb.at[i], dxm)
        b.pr[i, :, HI] = term(xp, 1, 2, m, 256, 256).astype(BF16)
        send("xb", (i, 0, 1), b.pr.at[i, :, HI], b.rr.at[i, :, HI], dxp)
        b.pl_[i, :, LO] = term(xm, 1, 2, m, 0, 256).astype(BF16)
        send("xb", (i, 1, 0), b.pl_.at[i, :, LO], b.rl.at[i, :, LO], dxm)
        for dx in range(4):
            a = b.mx[dx // 2, 0:KD, :]
            rows = pl.ds(pl.multiple_of((dx % 2) * 2048 + m * 512, 512), 512)
            b.q[i, dx] = lax.dot_general(a, b.h[rows, :], NT, preferred_element_type=F32).astype(BF16)
        lo, hi = b.q.at[i, pl.ds(0, 2)], b.q.at[i, pl.ds(2, 2)]

        @pl.when(rel == 2)
        def _():
            send("qa", (0,), lo, b.qa, dyp)
            send("qa", (1,), hi, b.qb, dym)

        @pl.when(rel == 1)
        def _():
            send("qb", (0, 1), hi, b.qr.at[pl.ds(2, 2)], dyp)

        @pl.when(rel == 3)
        def _():
            send("qb", (1, 0), lo, b.ql.at[pl.ds(0, 2)], dym)

    def part2(i):
        m, rel = rel_of(i)
        got("xa", (i, 0), b.ra.at[i])
        b.pr[i, :, LO] = (term(xp, 1, 2, m, 0, 256) + b.ra[i].astype(F32)).astype(BF16)
        send("xb", (i, 0, 0), b.pr.at[i, :, LO], b.rr.at[i, :, LO], dxp)
        got("xa", (i, 1), b.rb.at[i])
        b.pl_[i, :, HI] = (term(xm, 1, 2, m, 256, 256) + b.rb[i].astype(F32)).astype(BF16)
        send("xb", (i, 1, 1), b.pl_.at[i, :, HI], b.rl.at[i, :, HI], dxm)

        @pl.when(rel == 1)
        def _():
            got("qa", (0,), b.qa)
            for k in (0, 1):
                b.q[i, k] = (b.q[i, k].astype(F32) + b.qa[k].astype(F32)).astype(BF16)
            send("qb", (0, 0), b.q.at[i, pl.ds(0, 2)], b.qr.at[pl.ds(0, 2)], dyp)

        @pl.when(rel == 3)
        def _():
            got("qa", (1,), b.qb)
            for k in (0, 1):
                b.q[i, 2 + k] = (b.q[i, 2 + k].astype(F32) + b.qb[k].astype(F32)).astype(BF16)
            send("qb", (1, 1), b.q.at[i, pl.ds(2, 2)], b.ql.at[pl.ds(2, 2)], dym)

    def part3(i):
        m, rel = rel_of(i)
        for k, lanes in enumerate((LO, HI)):
            got("xb", (i, 0, k), b.rr.at[i, :, lanes])
            got("xb", (i, 1, k), b.rl.at[i, :, lanes])
            t = term(x, 1, 2, m, k * 256, 256) + b.rr[i, :, lanes].astype(F32) + b.rl[i, :, lanes].astype(F32)
            b.s[i, :, lanes] = t.astype(BF16)

            @pl.when(rel == 0)
            def _():
                b.sf[:, lanes] = t

        lo, hi = b.s.at[i, :, LO], b.s.at[i, :, HI]

        @pl.when(rel == 2)
        def _():
            send("ya", (0,), lo, b.ya, dyp)
            send("ya", (1,), hi, b.yb, dym)

        @pl.when(rel == 1)
        def _():
            send("yb", (0, 1), hi, b.yr.at[:, HI], dyp)

        @pl.when(rel == 3)
        def _():
            send("yb", (1, 0), lo, b.yl.at[:, LO], dym)

        @pl.when(rel == 0)
        def _():
            for k in (0, 1):
                got("qb", (0, k), b.qr.at[pl.ds(2 * k, 2)])
                got("qb", (1, k), b.ql.at[pl.ds(2 * k, 2)])

            @pl.loop(0, 4)
            def _(dx):
                t = b.q[i, dx].astype(F32) + b.qr[dx].astype(F32) + b.ql[dx].astype(F32)
                b.tq[dx] = t.astype(BF16)

                @pl.when(dx == x)
                def _():
                    b.tf[...] = t

            send("fa", (0,), b.tq.at[xo, :, LO], b.fa, dxp)
            send("fa", (1,), b.tq.at[xo, :, HI], b.fb, dxm)
            send("fb", (0, 1), b.tq.at[xp, :, HI], b.fr.at[:, HI], dxp)
            send("fb", (1, 0), b.tq.at[xm, :, LO], b.fl.at[:, LO], dxm)

    def part4(i):
        _, rel = rel_of(i)

        @pl.when(rel == 1)
        def _():
            got("ya", (0,), b.ya)
            b.s[i, :, LO] = (b.s[i, :, LO].astype(F32) + b.ya[...].astype(F32)).astype(BF16)
            send("yb", (0, 0), b.s.at[i, :, LO], b.yr.at[:, LO], dyp)

        @pl.when(rel == 3)
        def _():
            got("ya", (1,), b.yb)
            b.s[i, :, HI] = (b.s[i, :, HI].astype(F32) + b.yb[...].astype(F32)).astype(BF16)
            send("yb", (1, 1), b.s.at[i, :, HI], b.yl.at[:, HI], dym)

        @pl.when(rel == 0)
        def _():
            got("fa", (0,), b.fa)
            b.tq[xp, :, LO] = (b.tq[xp, :, LO].astype(F32) + b.fa[...].astype(F32)).astype(BF16)
            send("fb", (0, 0), b.tq.at[xp, :, LO], b.fr.at[:, LO], dxp)
            got("fa", (1,), b.fb)
            b.tq[xm, :, HI] = (b.tq[xm, :, HI].astype(F32) + b.fb[...].astype(F32)).astype(BF16)
            send("fb", (1, 1), b.tq.at[xm, :, HI], b.fl.at[:, HI], dxm)

    @pl.loop(0, 7)
    def _(t):
        @pl.when(t < 4)
        def _():
            h_step(t + 1)
            part1(t)

        @pl.when((t >= 1) & (t < 5))
        def _():
            part2(t - 1)

        @pl.when((t >= 2) & (t < 6))
        def _():
            part3(t - 2)

        @pl.when(t >= 3)
        def _():
            part4(t - 3)

    for lanes, k in ((LO, 0), (HI, 1)):
        got("yb", (0, k), b.yr.at[:, lanes])
        got("yb", (1, k), b.yl.at[:, lanes])
        got("fb", (0, k), b.fr.at[:, lanes])
        got("fb", (1, k), b.fl.at[:, lanes])
    for k, lanes in enumerate((LO, HI)):
        primal = b.tf[:, lanes] + b.fr[:, lanes].astype(F32) + b.fl[:, lanes].astype(F32)
        out[:, lanes] = primal.astype(BF16)
        tan = b.sf[:, lanes] + b.yr[:, lanes].astype(F32) + b.yl[:, lanes].astype(F32)
        sq = 1.0 / (1.0 + jnp.exp(-primal))
        slope = sq * (1.0 - sq)
        both = tan[:KD] * tan[:KD] + tan[KD:] * tan[KD:]
        b.cvs[0, :, lanes] = jnp.sum(slope * both, axis=0, keepdims=True)

    send("cv", (8,), b.cvs.at[0], b.cvr.at[8], dc)
    got("cv", (8,), b.cvr.at[8])
    b.cvs[1] = b.cvs[0] + b.cvr[8]
    send("cv", (9,), b.cvs.at[1], b.cvr.at[9], dxo)
    got("cv", (9,), b.cvr.at[9])
    b.cvs[2] = b.cvs[1] + b.cvr[9]
    for r in range(1, 8):
        send("cv", (r,), b.cvs.at[2], b.cvr.at[r], dev(z_=zs[r]))
    total = b.cvs[2]
    for r in range(1, 8):
        got("cv", (r,), b.cvr.at[r])
        total += b.cvr[r]
    curv[...] = total / (PROBES * D)

    for k in range(3):
        sent("tokx", (k,), tok)
        sent("m1", (k,), b.mx.at[0, pl.ds(0, KD), :])
    for d in (0, 1):
        for k in (0, 1):
            sent("toky", (d, k, 0), b.xg.at[0])
        sent("toky", (d, d, 1), b.xg.at[0])
        sent("w1", (d,), wchunk(X, z, 0))
        sent("qa", (d,), b.qa)
        sent("ya", (d,), b.ya)
        sent("fa", (d,), b.fa)
        for k in (0, 1):
            sent("qb", (d, k), b.qa)
            sent("yb", (d, k), b.ya)
            sent("fb", (d, k), b.fa)
    for sub in (0, 1):
        for r in range(8):
            sent("wd", (sub, r), b.w.at[wrows(X, z), :])
            sent("hd", (r, sub), hchunk(0, z))
        for s_ in range(4):
            for d in (0, 1):
                for half in (0, 1):
                    if s_ == 3 and half != d:
                        continue
                    sent("wr", (d, sub, s_, half), wchunk(X, z, 0))
                if s_ < 3 or sub == d:
                    sent("hr", (d, s_, sub), hchunk(0, z))
    for i in range(4):
        for d in (0, 1):
            sent("xa", (i, d), b.ra.at[0])
            for k in (0, 1):
                sent("xb", (i, d, k), b.ra.at[0])
    for r in range(1, 10):
        sent("cv", (r,), b.cvs.at[0])


def on_device(tokens, norm_gain, gate_weight, up_weight, down_weight, probes):
    vmem = pl.BlockSpec(memory_space=pltpu.VMEM)
    sems = []
    for shape in SEMS.values():
        sems += [pltpu.SemaphoreType.DMA(shape), pltpu.SemaphoreType.DMA(shape)]
    out, curv = pl.pallas_call(
        kernel,
        out_shape=(jax.ShapeDtypeStruct((KD, 512), BF16), jax.ShapeDtypeStruct((1, 512), F32)),
        in_specs=[vmem] * 6,
        out_specs=(vmem, vmem),
        scratch_shapes=[pltpu.VMEM(s, t) for s, t in SCRATCH.values()] + sems + [pltpu.SemaphoreType.DMA((6,))],
        compiler_params=pltpu.CompilerParams(
            collective_id=0, has_side_effects=True, vmem_limit_bytes=60 * 1024 * 1024
        ),
        name="mlp_curv",
    )(tokens, norm_gain.astype(F32).reshape(8, DT), gate_weight, up_weight, down_weight, probes)
    return out.T, curv.reshape(512)


def solution(mesh):
    return jax.shard_map(
        on_device,
        mesh=mesh,
        in_specs=(
            P("fsdp", "tp"),
            P(),
            P("fsdp", "tp"),
            P("fsdp", "tp"),
            P("fsdp", "tp"),
            P(None, "fsdp", "tp"),
        ),
        out_specs=(P("tp", "fsdp"), P("tp")),
        check_vma=False,
    )
```

```python
import jax
import jax.numpy as jnp
from jax import lax
from jax.experimental import pallas as pl
from jax.experimental.pallas import tpu as pltpu
from jax.sharding import PartitionSpec as P

MESH = pl.DeviceIdType.MESH
F32, BF16 = jnp.float32, jnp.bfloat16
D = 3584
PROBES = 2
EPS = 1e-06
KD = 112
FH = 640
TB = 128
DT = 448
XR = 224
NT = (((1,), (1,)), ((), ()))

SCRATCH = dict(
    xg=((8, 256, DT), BF16),
    xn=((8, 256, DT), BF16),
    g8=((8, DT), F32),
    w=((D, 2 * FH), BF16),
    acc=((256, 2 * FH), F32),
    h=((4096, FH), BF16),
    mx=((2, 3 * KD, FH), BF16),
    popp=((8, XR, 256), BF16),
    pr=((8, XR, 256), BF16),
    pl_=((8, XR, 256), BF16),
    dr=((8, XR, 128), F32),
    dl=((8, XR, 128), F32),
    ra=((8, XR, 128), BF16),
    rb=((8, XR, 128), BF16),
    rr=((8, XR, 256), BF16),
    rl=((8, XR, 256), BF16),
    s=((8, XR, 256), BF16),
    sf=((2, XR, 256), F32),
    ya=((2, XR, 128), BF16),
    yb=((2, XR, 128), BF16),
    yr=((2, XR, 256), BF16),
    yl=((2, XR, 256), BF16),
    q=((8, 4, KD, 256), BF16),
    qa=((2, 2, KD, 256), BF16),
    qb=((2, 2, KD, 256), BF16),
    qr=((2, 4, KD, 256), BF16),
    ql=((2, 4, KD, 256), BF16),
    tq=((2, 4, KD, 256), BF16),
    tf=((2, KD, 256), F32),
    fa=((2, KD, 128), BF16),
    fb=((2, KD, 128), BF16),
    fr=((2, KD, 256), BF16),
    fl=((2, KD, 256), BF16),
    cvs=((1, 512), F32),
    cvr=((32, 1, 512), F32),
)
SEMS = dict(
    tokx=(3,), toky=(2, 2, 2), w1=(2,), m1=(3,), wr=(2, 2, 4, 2), wd=(2, 8), hr=(2, 4, 2), hd=(8, 2),
    xa=(8, 2), xb=(8, 2, 2), qa=(2, 2), qb=(2, 2, 2), ya=(2, 2), yb=(2, 2, 2), fa=(2, 2), fb=(2, 2, 2), cv=(32,),
)


class Refs:
    pass


def kernel(tok_t, gain, wg, wu, dn, pr, out, curv, *scratch):
    b, ss, rs = Refs(), Refs(), Refs()
    names = list(SCRATCH)
    for n, r in zip(names, scratch):
        setattr(b, n, r)
    rest = scratch[len(names):]
    for i, n in enumerate(SEMS):
        setattr(ss, n, rest[2 * i])
        setattr(rs, n, rest[2 * i + 1])
    loc = rest[2 * len(SEMS)]

    fi, ti = lax.axis_index("fsdp"), lax.axis_index("tp")
    X, z, c = fi // 16, lax.rem(fi // 2, 8), lax.rem(fi, 2)
    xl, y = ti // 4, lax.rem(ti, 4)
    x = X * 2 + xl

    def dev(x_=None, y_=None, z_=None, c_=None):
        x_ = x if x_ is None else x_
        y_ = y if y_ is None else y_
        z_ = z if z_ is None else z_
        c_ = c if c_ is None else c_
        return ((x_ // 2) * 16 + z_ * 2 + c_, lax.rem(x_, 2) * 4 + y_)

    xp, xm, xo = lax.rem(x + 1, 4), lax.rem(x + 3, 4), lax.rem(x + 2, 4)
    yp, ym = lax.rem(y + 1, 4), lax.rem(y + 3, 4)
    dxp, dxm, dxo = dev(x_=xp), dev(x_=xm), dev(x_=xo)
    dyp, dym = dev(y_=yp), dev(y_=ym)
    dz = (dev(z_=lax.rem(z + 1, 8)), dev(z_=lax.rem(z + 7, 8)))
    dc = dev(c_=1 - c)

    def copy(name, idx, src, dst, to):
        return pltpu.make_async_remote_copy(
            src_ref=src, dst_ref=dst, send_sem=getattr(ss, name).at[idx], recv_sem=getattr(rs, name).at[idx],
            device_id=to, device_id_type=MESH,
        )

    def send(name, idx, src, dst, to):
        copy(name, idx, src, dst, to).start()

    def got(name, idx, ref):
        copy(name, idx, ref, ref, dc).wait_recv()

    def sent(name, idx, ref):
        copy(name, idx, ref, ref, dc).wait_send()

    def cols(k):
        return pl.ds(pl.multiple_of(k * FH, 128), FH)

    def wrows(X_, z_, c_=None):
        c_ = c if c_ is None else c_
        return pl.ds(pl.multiple_of((X_ * 16 + z_ * 2 + c_) * KD, 16), KD)

    def wchunk(X_, z_, half):
        return b.w.at[wrows(X_, z_), pl.ds(half * FH, FH)]

    def hchunk(X_, z_):
        return b.h.at[pl.ds(pl.multiple_of((X_ * 16 + z_ * 2 + c) * TB, 128), TB), :]

    mine = [
        (wg.at[:, cols(X)], wchunk(X, z, 0)),
        (wu.at[:, cols(X)], wchunk(X, z, 1)),
        (dn.at[:, cols(X)], b.mx.at[X, pl.ds(0, KD), :]),
        (pr.at[0, :, cols(X)], b.mx.at[X, pl.ds(KD, KD), :]),
        (pr.at[1, :, cols(X)], b.mx.at[X, pl.ds(2 * KD, KD), :]),
    ]
    own = [pltpu.make_async_copy(s_, d_, loc.at[i]) for i, (s_, d_) in enumerate(mine)]
    for o in own:
        o.start()

    tx = b.xg.at[ti, pl.ds(pl.multiple_of(X * TB, 128), TB), :]
    tx[...] = tok_t[...].T
    for j in range(8):
        at = j * DT
        while at < (j + 1) * DT:
            n = min(128 - at % 128, (j + 1) * DT - at)
            row, lane = at // 128, at % 128
            b.g8[j : j + 1, at - j * DT : at - j * DT + n] = gain[row : row + 1, lane : lane + n].astype(F32)
            at += n

    barrier = pltpu.get_barrier_semaphore()
    peers = [(lax.rem(fi + r, 32), ti) for r in range(1, 32)]
    partners = [dxp, dxm, dyp, dym] + peers
    for p in partners:
        pl.semaphore_signal(barrier, inc=1, device_id=p, device_id_type=MESH)
    pl.semaphore_wait(barrier, len(partners))

    for o in own:
        o.wait()

    def ring_start(sub, X_):
        for half in (0, 1):
            for d in (0, 1):
                send("wr", (d, sub, 0, half), wchunk(X_, z, half), wchunk(X_, z, half), dz[d])
        send("wd", (sub, 0), b.w.at[wrows(X_, z), :], b.w.at[wrows(X_, z), :], dc)

    ring_start(0, X)
    for k, to in enumerate((dxp, dxm, dxo)):
        send("tokx", (k,), tx, tx, to)
    for half, src in enumerate((wg, wu)):
        send("w1", (half,), src.at[:, cols(1 - X)], wchunk(X, z, half), dxo)

    def m_send():
        for k, src in enumerate((dn, pr.at[0], pr.at[1])):
            send("m1", (k,), src.at[:, cols(1 - X)], b.mx.at[X, pl.ds(k * KD, KD), :], dxo)

    def zsrc(d, s_):
        return lax.rem(z + (8 - s_ if d == 0 else s_), 8)

    def ring_step(sub, X_, s_):
        for half in (0, 1):
            for d in (0, 1):
                if s_ == 4 and half != d:
                    continue
                ch = wchunk(X_, zsrc(d, s_), half)
                got("wr", (d, sub, s_ - 1, half), ch)
                if s_ < 3 or (s_ == 3 and half == d):
                    send("wr", (d, sub, s_, half), ch, ch, dz[d])
        for d in (0, 1):
            if s_ == 4 and d == 1:
                continue
            blk = b.w.at[wrows(X_, zsrc(d, s_)), :]
            send("wd", (sub, 8 - s_ if d == 0 else s_), blk, blk, dc)

    par = lax.rem(z, 2)

    def pair(i):
        f = 3 * i - 5 * (i // 2) - 2 * (i // 3)
        return lax.rem(z // 2 + f * (1 - par) + (4 - f) * par, 4)

    def other_core(sub, X_, s_):
        if s_ == 1:
            got("wd", (sub, 0), b.w.at[wrows(X_, z, 1 - c), :])
        for d in (0, 1):
            if s_ == 4 and d == 1:
                continue
            got("wd", (sub, 8 - s_ if d == 0 else s_), b.w.at[wrows(X_, zsrc(d, s_), 1 - c), :])

    def multiply(X_, s_):
        j = X_ * 4 + pair(s_ - 1)

        @pl.loop(0, 5)
        def _(n):
            cs = pl.ds(pl.multiple_of(n * 256, 256), 256)
            ks = pl.ds(pl.multiple_of(j * DT, 64), DT)
            b.acc[:, cs] += jnp.dot(b.xn[j], b.w[ks, cs], preferred_element_type=F32)

    def tokx_done():
        for k, sx in enumerate((xm, xp, xo)):
            got("tokx", (k,), b.xg.at[lax.rem(sx, 2) * 4 + y, pl.ds(pl.multiple_of((sx // 2) * TB, 128), TB), :])
        for k in (0, 1):
            blk = b.xg.at[k * 4 + y]
            send("toky", (0, k, 0), blk, blk, dyp)
            send("toky", (1, k, 0), blk, blk, dym)

    def toky_first():
        for d, sy, to in ((0, ym, dyp), (1, yp, dym)):
            for k in (0, 1):
                got("toky", (d, k, 0), b.xg.at[k * 4 + sy])
            blk = b.xg.at[d * 4 + sy]
            send("toky", (d, d, 1), blk, blk, to)

    def toky_last():
        for d in (0, 1):
            got("toky", (d, d, 1), b.xg.at[d * 4 + lax.rem(y + 2, 4)])

    def norm():
        @pl.loop(0, 8)
        def _(t):
            rows = pl.ds(pl.multiple_of(t * 32, 32), 32)
            total = jnp.zeros((32, 1), F32)
            for j in range(8):
                v = b.xg[j, rows, :].astype(F32)
                total += jnp.sum(v * v, axis=1, keepdims=True)
            inv = lax.rsqrt(total / D + EPS)
            for j in range(8):
                v = b.xg[j, rows, :].astype(F32)
                b.xn[j, rows, :] = (v * inv * b.g8[j : j + 1, :]).astype(BF16)

    b.acc[...] = jnp.zeros_like(b.acc)
    ring_step(0, X, 1)
    tokx_done()
    ring_step(0, X, 2)
    ring_step(0, X, 3)
    for half in (0, 1):
        got("w1", (half,), wchunk(1 - X, z, half))
    ring_start(1, 1 - X)
    toky_first()
    m_send()
    ring_step(0, X, 4)
    toky_last()
    norm()
    for s_ in (1, 2):
        other_core(0, X, s_)
        multiply(X, s_)
    ring_step(1, 1 - X, 1)
    for s_ in (3, 4):
        other_core(0, X, s_)
        multiply(X, s_)
    ring_step(1, 1 - X, 2)
    other_core(1, 1 - X, 1)
    multiply(1 - X, 1)
    ring_step(1, 1 - X, 3)
    for s_ in (2, 3):
        other_core(1, 1 - X, s_)
        multiply(1 - X, s_)
    ring_step(1, 1 - X, 4)
    other_core(1, 1 - X, 4)
    multiply(1 - X, 4)

    @pl.loop(0, 5)
    def _(n):
        cs = pl.ds(pl.multiple_of(n * 128, 128), 128)
        g = b.acc[:, cs]
        u = b.acc[:, pl.ds(pl.multiple_of(FH + n * 128, 128), 128)]
        hid = (g / (1.0 + jnp.exp(-g)) * u).astype(BF16)
        for k in (0, 1):
            b.h[pl.ds(pl.multiple_of((k * 16 + z * 2 + c) * TB, 128), TB), cs] = hid[k * TB : (k + 1) * TB]

    for k in (0, 1):
        for d in (0, 1):
            send("hr", (d, 0, k), hchunk(k, z), hchunk(k, z), dz[d])
        send("hd", (0, k), hchunk(k, z), hchunk(k, z), dc)
    for k in range(3):
        got("m1", (k,), b.mx.at[1 - X, pl.ds(k * KD, KD), :])

    def hother(k, z_):
        return b.h.at[pl.ds(pl.multiple_of((k * 16 + z_ * 2 + 1 - c) * TB, 128), TB), :]

    def h_take(s_):
        for k in (0, 1):
            for d in (0, 1):
                zz = lax.rem(z + (8 - s_ if d == 0 else s_), 8)
                r = 8 - s_ if d == 0 else s_
                ch = hchunk(k, zz)

                def take():
                    got("hr", (d, s_ - 1, k), ch)

                    @pl.when(s_ < (4 if k == d else 3))
                    def _():
                        send("hr", (d, s_, k), ch, ch, dz[d])

                    send("hd", (r, k), ch, ch, dc)

                if k == d:
                    take()
                else:
                    pl.when(s_ < 4)(take)

    def level(i):
        k = (i + 1) // 2
        r = lax.rem(i, 2) * (8 - 2 * k) + k
        return lax.rem(r, 8), lax.rem(z + r, 8)

    def term(dx, k0, nk, zz):
        a = b.mx[dx // 2, k0 * KD : (k0 + nk) * KD, :]
        rows = pl.ds(pl.multiple_of(lax.rem(dx, 2) * 2048 + zz * 256, 256), 256)
        return lax.dot_general(a, b.h[rows, :], NT, preferred_element_type=F32)

    LO, HI = pl.ds(0, 128), pl.ds(128, 128)
    HALVES = ((0, LO), (1, HI))

    def place(i):
        _, zz = level(i)
        return zz, lax.rem(zz, 2), lax.rem(zz // 2 - y + 4, 4)

    def plus(u, v):
        return (u.astype(F32) + v.astype(F32)).astype(BF16)

    def part1(i):
        zz, e, rel = place(i)
        r, _ = level(i)
        for k in (0, 1):
            got("hd", (r, k), hother(k, zz))
        b.popp[i] = term(xo, 1, 2, zz).astype(BF16)
        send("xa", (i, 0), b.popp.at[i, :, LO], b.ra.at[i], dxp)
        send("xa", (i, 1), b.popp.at[i, :, HI], b.rb.at[i], dxm)
        t = term(xp, 1, 2, zz)
        b.pr[i, :, HI] = t[:, 128:].astype(BF16)
        send("xb", (i, 0, 1), b.pr.at[i, :, HI], b.rr.at[i, :, HI], dxp)
        b.dr[i] = t[:, :128]
        t = term(xm, 1, 2, zz)
        b.pl_[i, :, LO] = t[:, :128].astype(BF16)
        send("xb", (i, 1, 0), b.pl_.at[i, :, LO], b.rl.at[i, :, LO], dxm)
        b.dl[i] = t[:, 128:]
        for dx in range(4):
            b.q[i, dx] = term(dx, 0, 1, zz).astype(BF16)
        lo, hi = b.q.at[i, pl.ds(0, 2)], b.q.at[i, pl.ds(2, 2)]

        @pl.when(rel == 2)
        def _():
            send("qa", (e, 0), lo, b.qa.at[e], dyp)
            send("qa", (e, 1), hi, b.qb.at[e], dym)

        @pl.when(rel == 1)
        def _():
            send("qb", (e, 0, 1), hi, b.qr.at[e, pl.ds(2, 2)], dyp)

        @pl.when(rel == 3)
        def _():
            send("qb", (e, 1, 0), lo, b.ql.at[e, pl.ds(0, 2)], dym)

    def part2(i):
        zz, e, rel = place(i)
        got("xa", (i, 0), b.ra.at[i])
        b.pr[i, :, LO] = (b.dr[i] + b.ra[i].astype(F32)).astype(BF16)
        send("xb", (i, 0, 0), b.pr.at[i, :, LO], b.rr.at[i, :, LO], dxp)
        got("xa", (i, 1), b.rb.at[i])
        b.pl_[i, :, HI] = (b.dl[i] + b.rb[i].astype(F32)).astype(BF16)
        send("xb", (i, 1, 1), b.pl_.at[i, :, HI], b.rl.at[i, :, HI], dxm)

        @pl.when(rel == 1)
        def _():
            got("qa", (e, 0), b.qa.at[e])
            for k in (0, 1):
                b.q[i, k] = plus(b.q[i, k], b.qa[e, k])
            send("qb", (e, 0, 0), b.q.at[i, pl.ds(0, 2)], b.qr.at[e, pl.ds(0, 2)], dyp)

        @pl.when(rel == 3)
        def _():
            got("qa", (e, 1), b.qb.at[e])
            for k in (0, 1):
                b.q[i, 2 + k] = plus(b.q[i, 2 + k], b.qb[e, k])
            send("qb", (e, 1, 1), b.q.at[i, pl.ds(2, 2)], b.ql.at[e, pl.ds(2, 2)], dym)

    def part3(i):
        zz, e, rel = place(i)
        for k, lanes in HALVES:
            got("xb", (i, 0, k), b.rr.at[i, :, lanes])
            got("xb", (i, 1, k), b.rl.at[i, :, lanes])
        t = term(x, 1, 2, zz) + b.rr[i].astype(F32) + b.rl[i].astype(F32)
        b.s[i] = t.astype(BF16)
        lo, hi = b.s.at[i, :, LO], b.s.at[i, :, HI]

        @pl.when(rel == 2)
        def _():
            send("ya", (e, 0), lo, b.ya.at[e], dyp)
            send("ya", (e, 1), hi, b.yb.at[e], dym)

        @pl.when(rel == 1)
        def _():
            send("yb", (e, 0, 1), hi, b.yr.at[e, :, HI], dyp)

        @pl.when(rel == 3)
        def _():
            send("yb", (e, 1, 0), lo, b.yl.at[e, :, LO], dym)

        @pl.when(rel == 0)
        def _():
            b.sf[e] = t
            for k in (0, 1):
                got("qb", (e, 0, k), b.qr.at[e, pl.ds(2 * k, 2)])
                got("qb", (e, 1, k), b.ql.at[e, pl.ds(2 * k, 2)])

            @pl.loop(0, 4)
            def _(dx):
                u = b.q[i, dx].astype(F32) + b.qr[e, dx].astype(F32) + b.ql[e, dx].astype(F32)
                b.tq[e, dx] = u.astype(BF16)

                @pl.when(dx == x)
                def _():
                    b.tf[e] = u

            send("fa", (e, 0), b.tq.at[e, xo, :, LO], b.fa.at[e], dxp)
            send("fa", (e, 1), b.tq.at[e, xo, :, HI], b.fb.at[e], dxm)
            send("fb", (e, 0, 1), b.tq.at[e, xp, :, HI], b.fr.at[e, :, HI], dxp)
            send("fb", (e, 1, 0), b.tq.at[e, xm, :, LO], b.fl.at[e, :, LO], dxm)

    def part4(i):
        _, e, rel = place(i)

        @pl.when(rel == 1)
        def _():
            got("ya", (e, 0), b.ya.at[e])
            b.s[i, :, LO] = plus(b.s[i, :, LO], b.ya[e])
            send("yb", (e, 0, 0), b.s.at[i, :, LO], b.yr.at[e, :, LO], dyp)

        @pl.when(rel == 3)
        def _():
            got("ya", (e, 1), b.yb.at[e])
            b.s[i, :, HI] = plus(b.s[i, :, HI], b.yb[e])
            send("yb", (e, 1, 1), b.s.at[i, :, HI], b.yl.at[e, :, HI], dym)

        @pl.when(rel == 0)
        def _():
            got("fa", (e, 0), b.fa.at[e])
            b.tq[e, xp, :, LO] = plus(b.tq[e, xp, :, LO], b.fa[e])
            send("fb", (e, 0, 0), b.tq.at[e, xp, :, LO], b.fr.at[e, :, LO], dxp)
            got("fa", (e, 1), b.fb.at[e])
            b.tq[e, xm, :, HI] = plus(b.tq[e, xm, :, HI], b.fb[e])
            send("fb", (e, 1, 1), b.tq.at[e, xm, :, HI], b.fl.at[e, :, HI], dxm)

    LAG2, LAG3, LAG4 = 1, 2, 3

    @pl.loop(0, 8 + LAG4)
    def _(t):
        @pl.when((lax.rem(t, 2) == 1) & (t < 8))
        def _():
            h_take((t + 1) // 2)

        @pl.when(t < 8)
        def _():
            part1(t)

        @pl.when((t >= LAG2) & (t < 8 + LAG2))
        def _():
            part2(t - LAG2)

        @pl.when((t >= LAG3) & (t < 8 + LAG3))
        def _():
            part3(t - LAG3)

        @pl.when(t >= LAG4)
        def _():
            part4(t - LAG4)

    for e in (0, 1):
        for k, lanes in HALVES:
            got("yb", (e, 0, k), b.yr.at[e, :, lanes])
            got("yb", (e, 1, k), b.yl.at[e, :, lanes])
            got("fb", (e, 0, k), b.fr.at[e, :, lanes])
            got("fb", (e, 1, k), b.fl.at[e, :, lanes])
        primal = b.tf[e] + b.fr[e].astype(F32) + b.fl[e].astype(F32)
        out[:, e * 256 : (e + 1) * 256] = primal.astype(BF16)
        tan = b.sf[e] + b.yr[e].astype(F32) + b.yl[e].astype(F32)
        sq = 1.0 / (1.0 + jnp.exp(-primal))
        slope = sq * (1.0 - sq)
        both = tan[:KD] * tan[:KD] + tan[KD:] * tan[KD:]
        b.cvs[:, e * 256 : (e + 1) * 256] = jnp.sum(slope * both, axis=0, keepdims=True)

    for r in range(1, 32):
        send("cv", (r,), b.cvs, b.cvr.at[r], peers[r - 1])
    total = b.cvs[...]
    for r in range(1, 32):
        got("cv", (r,), b.cvr.at[r])
        total += b.cvr[r]
    curv[...] = total / (PROBES * D)

    for k in range(3):
        sent("tokx", (k,), tx)
        sent("m1", (k,), b.mx.at[0, pl.ds(0, KD), :])
    for d in (0, 1):
        for k in (0, 1):
            sent("toky", (d, k, 0), b.xg.at[0])
        sent("toky", (d, d, 1), b.xg.at[0])
        sent("w1", (d,), wchunk(X, z, 0))
        for e in (0, 1):
            sent("qa", (e, d), b.qa.at[0])
            sent("ya", (e, d), b.ya.at[0])
            sent("fa", (e, d), b.fa.at[0])
            for k in (0, 1):
                sent("qb", (e, d, k), b.qa.at[0])
                sent("yb", (e, d, k), b.ya.at[0])
                sent("fb", (e, d, k), b.fa.at[0])
    for sub in (0, 1):
        for r in range(8):
            sent("wd", (sub, r), b.w.at[wrows(X, z), :])
            sent("hd", (r, sub), hchunk(0, z))
        for s_ in range(4):
            for d in (0, 1):
                for half in (0, 1):
                    if s_ == 3 and half != d:
                        continue
                    sent("wr", (d, sub, s_, half), wchunk(X, z, 0))
                if s_ < 3 or sub == d:
                    sent("hr", (d, s_, sub), hchunk(0, z))
    for i in range(8):
        for d in (0, 1):
            sent("xa", (i, d), b.ra.at[0])
            for k in (0, 1):
                sent("xb", (i, d, k), b.ra.at[0])
    for r in range(1, 32):
        sent("cv", (r,), b.cvs)


def on_device(tokens, norm_gain, gate_weight, up_weight, down_weight, probes):
    vmem = pl.BlockSpec(memory_space=pltpu.VMEM)
    sems = []
    for shape in SEMS.values():
        sems += [pltpu.SemaphoreType.DMA(shape), pltpu.SemaphoreType.DMA(shape)]
    out, curv = pl.pallas_call(
        kernel,
        out_shape=(jax.ShapeDtypeStruct((KD, 512), BF16), jax.ShapeDtypeStruct((1, 512), F32)),
        in_specs=[vmem] * 6,
        out_specs=(vmem, vmem),
        scratch_shapes=[pltpu.VMEM(s, t) for s, t in SCRATCH.values()] + sems + [pltpu.SemaphoreType.DMA((5,))],
        compiler_params=pltpu.CompilerParams(
            collective_id=0, has_side_effects=True, vmem_limit_bytes=60 * 1024 * 1024
        ),
        name="mlp_curv",
    )(tokens.T, norm_gain.reshape(28, 128), gate_weight, up_weight, down_weight, probes)
    return out.T, curv.reshape(512)


def solution(mesh):
    return jax.shard_map(
        on_device,
        mesh=mesh,
        in_specs=(
            P("fsdp", "tp"),
            P(),
            P("fsdp", "tp"),
            P("fsdp", "tp"),
            P("fsdp", "tp"),
            P(None, "fsdp", "tp"),
        ),
        out_specs=(P("tp", "fsdp"), P("tp")),
        check_vma=False,
    )
```

```python
import jax
import jax.numpy as jnp
from jax import lax
from jax.experimental import pallas as pl
from jax.experimental.pallas import tpu as pltpu
from jax.sharding import PartitionSpec as P

MESH = pl.DeviceIdType.MESH
F32, BF16 = jnp.float32, jnp.bfloat16
D = 3584
PROBES = 2
EPS = 1e-06
KD = 112
FH = 640
TB = 128
DT = 448
NY, NX = 2 * KD, KD

SCRATCH = dict(
    xg=((8, 256, DT), BF16),
    xn=((8, 256, DT), BF16),
    g8=((8, DT), F32),
    w=((D, 2 * FH), BF16),
    acc=((256, 2 * FH), F32),
    hs=((2, FH, TB), BF16),
    h=((32, FH, TB), BF16),
    mx=((2, 3 * KD, 2 * FH), BF16),
    px=((8, 2, NX, TB), BF16),
    rx=((8, 2, NX, TB), BF16),
    sx=((8, 2, NX, TB), F32),
    s=((8, 2, NX, TB), BF16),
    ya=((2, NX, TB), BF16),
    yb=((2, NX, TB), BF16),
    yr=((2, 2, NX, TB), BF16),
    yl=((2, 2, NX, TB), BF16),
    us=((2, 2, NX, TB), BF16),
    fs=((2, 2, NX, TB), BF16),
    q=((8, 2, 2, NY, TB), BF16),
    qa=((2, 2, NY, TB), BF16),
    qb=((2, 2, NY, TB), BF16),
    qr=((2, 2, 2, NY, TB), BF16),
    ql=((2, 2, 2, NY, TB), BF16),
    tq=((2, 2, 2, NY, TB), BF16),
    fq=((4, 2, NY, TB), BF16),
    ov=((KD, 512), BF16),
    cvo=((1, 512), F32),
    cvs=((1, 512), F32),
    cvr=((32, 1, 512), F32),
)
SEMS = dict(
    tokx=(3,), toky=(2, 2, 2), w1=(1,), m1=(1,), wr=(2, 2, 4, 2), wd=(2, 8), hx=(2,), hr=(2, 4, 2), hd=(8, 2),
    px=(8,), qa=(2, 2), qr=(2, 2), ya=(2, 2), yr=(2, 2), fq=(2,), fs=(2,), cv=(1,),
)


class Refs:
    pass


def kernel(tok_t, gain, wg, wu, dn, pr, out, curv, *scratch):
    b, ss, rs = Refs(), Refs(), Refs()
    names = list(SCRATCH)
    for n, r in zip(names, scratch):
        setattr(b, n, r)
    rest = scratch[len(names):]
    for i, n in enumerate(SEMS):
        setattr(ss, n, rest[2 * i])
        setattr(rs, n, rest[2 * i + 1])
    loc = rest[2 * len(SEMS)]

    fi, ti = lax.axis_index("fsdp"), lax.axis_index("tp")
    X, z, c = fi // 16, lax.rem(fi // 2, 8), lax.rem(fi, 2)
    xl, y = ti // 4, lax.rem(ti, 4)
    x = X * 2 + xl

    def dev(x_=None, y_=None, z_=None, c_=None):
        x_ = x if x_ is None else x_
        y_ = y if y_ is None else y_
        z_ = z if z_ is None else z_
        c_ = c if c_ is None else c_
        return ((x_ // 2) * 16 + z_ * 2 + c_, lax.rem(x_, 2) * 4 + y_)

    xp, xm, xo = lax.rem(x + 1, 4), lax.rem(x + 3, 4), lax.rem(x + 2, 4)
    yp, ym = lax.rem(y + 1, 4), lax.rem(y + 3, 4)
    dxp, dxm, dxo = dev(x_=xp), dev(x_=xm), dev(x_=xo)
    dyp, dym = dev(y_=yp), dev(y_=ym)
    dz = (dev(z_=lax.rem(z + 1, 8)), dev(z_=lax.rem(z + 7, 8)))
    dc = dev(c_=1 - c)

    def copy(name, idx, src, dst, to):
        out_sem = getattr(ss, name).at[idx[0] if name == "tokx" else 0]
        return pltpu.make_async_remote_copy(
            src_ref=src, dst_ref=dst, send_sem=out_sem, recv_sem=getattr(rs, name).at[idx],
            device_id=to, device_id_type=MESH,
        )

    def send(name, idx, src, dst, to):
        copy(name, idx, src, dst, to).start()

    def got(name, idx, ref):
        copy(name, idx, ref, ref, dc).wait_recv()

    def sent(name, ref, idx=0):
        copy(name, (idx,) + (0,) * (len(SEMS[name]) - 1), ref, ref, dc).wait_send()

    def cols(k):
        return pl.ds(pl.multiple_of(k * FH, 128), FH)

    def wrows(X_, z_, c_=None):
        c_ = c if c_ is None else c_
        return pl.ds(pl.multiple_of((X_ * 16 + z_ * 2 + c_) * KD, 16), KD)

    def wchunk(X_, z_, half):
        return b.w.at[wrows(X_, z_), pl.ds(half * FH, FH)]

    def hchunk(X_, z_):
        return b.h.at[c * 16 + X_ * 8 + z_]

    mine = [
        (wg.at[:, cols(X)], wchunk(X, z, 0)),
        (wu.at[:, cols(X)], wchunk(X, z, 1)),
        (dn, b.mx.at[X, pl.ds(0, KD), :]),
        (pr.at[0], b.mx.at[X, pl.ds(KD, KD), :]),
        (pr.at[1], b.mx.at[X, pl.ds(2 * KD, KD), :]),
    ]
    own = [pltpu.make_async_copy(s_, d_, loc.at[i]) for i, (s_, d_) in enumerate(mine)]
    for o in own:
        o.start()

    tx = b.xg.at[ti, pl.ds(pl.multiple_of(X * TB, 128), TB), :]
    tx[...] = tok_t[...].T
    for j in range(8):
        at = j * DT
        while at < (j + 1) * DT:
            n = min(128 - at % 128, (j + 1) * DT - at)
            row, lane = at // 128, at % 128
            b.g8[j : j + 1, at - j * DT : at - j * DT + n] = gain[row : row + 1, lane : lane + n].astype(F32)
            at += n

    barrier = pltpu.get_barrier_semaphore()
    peers = [(lax.rem(fi + r, 32), ti) for r in range(1, 32)]
    partners = [dxp, dxm, dyp, dym] + peers
    for p in partners:
        pl.semaphore_signal(barrier, inc=1, device_id=p, device_id_type=MESH)
    pl.semaphore_wait(barrier, len(partners))

    for o in own:
        o.wait()

    def ring_start(sub, X_):
        for half in (0, 1):
            for d in (0, 1):
                send("wr", (d, sub, 0, half), wchunk(X_, z, half), wchunk(X_, z, half), dz[d])
        send("wd", (sub, 0), b.w.at[wrows(X_, z), :], b.w.at[wrows(X_, z), :], dc)

    ring_start(0, X)
    for k, to in enumerate((dxp, dxm, dxo)):
        send("tokx", (k,), tx, tx, to)
    for half, src in enumerate((wg, wu)):
        send("w1", (0,), src.at[:, cols(1 - X)], wchunk(X, z, half), dxo)

    def m_send():
        for k, src in enumerate((dn, pr.at[0], pr.at[1])):
            send("m1", (0,), src, b.mx.at[X, pl.ds(k * KD, KD), :], dxo)

    def zsrc(d, s_):
        return lax.rem(z + (8 - s_ if d == 0 else s_), 8)

    def ring_half(sub, X_, s_, half):
        for d in (0, 1):
            if s_ == 4 and half != d:
                continue
            ch = wchunk(X_, zsrc(d, s_), half)
            got("wr", (d, sub, s_ - 1, half), ch)
            if s_ < 3 or (s_ == 3 and half == d):
                send("wr", (d, sub, s_, half), ch, ch, dz[d])
        if half == 1:
            for d in (0, 1):
                if s_ == 4 and d == 1:
                    continue
                blk = b.w.at[wrows(X_, zsrc(d, s_)), :]
                send("wd", (sub, 8 - s_ if d == 0 else s_), blk, blk, dc)

    par = lax.rem(z, 2)

    def pair(i):
        f = 3 * i - 5 * (i // 2) - 2 * (i // 3)
        return lax.rem(z // 2 + f * (1 - par) + (4 - f) * par, 4)

    def other_core(sub, X_, s_):
        if s_ == 1:
            got("wd", (sub, 0), b.w.at[wrows(X_, z, 1 - c), :])
        for d in (0, 1):
            if s_ == 4 and d == 1:
                continue
            got("wd", (sub, 8 - s_ if d == 0 else s_), b.w.at[wrows(X_, zsrc(d, s_), 1 - c), :])

    def multiply(X_, s_):
        j = X_ * 4 + pair(s_ - 1)

        @pl.loop(0, 5)
        def _(n):
            cs = pl.ds(pl.multiple_of(n * 256, 256), 256)
            ks = pl.ds(pl.multiple_of(j * DT, 64), DT)
            b.acc[:, cs] += jnp.dot(b.xn[j], b.w[ks, cs], preferred_element_type=F32)

    def tokx_done():
        for k, sx in enumerate((xm, xp, xo)):
            got("tokx", (k,), b.xg.at[lax.rem(sx, 2) * 4 + y, pl.ds(pl.multiple_of((sx // 2) * TB, 128), TB), :])
        for k in (0, 1):
            blk = b.xg.at[k * 4 + y]
            send("toky", (0, k, 0), blk, blk, dyp)
            send("toky", (1, k, 0), blk, blk, dym)

    def toky_first():
        for d, sy, to in ((0, ym, dyp), (1, yp, dym)):
            for k in (0, 1):
                got("toky", (d, k, 0), b.xg.at[k * 4 + sy])
            blk = b.xg.at[d * 4 + sy]
            send("toky", (d, d, 1), blk, blk, to)

    def toky_last():
        for d in (0, 1):
            got("toky", (d, d, 1), b.xg.at[d * 4 + lax.rem(y + 2, 4)])

    def norm():
        @pl.loop(0, 8)
        def _(t):
            rows = pl.ds(pl.multiple_of(t * 32, 32), 32)
            total = jnp.zeros((32, 1), F32)
            for j in range(8):
                v = b.xg[j, rows, :].astype(F32)
                total += jnp.sum(v * v, axis=1, keepdims=True)
            inv = lax.rsqrt(total / D + EPS)
            for j in range(8):
                v = b.xg[j, rows, :].astype(F32)
                b.xn[j, rows, :] = (v * inv * b.g8[j : j + 1, :]).astype(BF16)

    b.acc[...] = jnp.zeros_like(b.acc)
    ring_half(0, X, 1, 0)
    tokx_done()
    ring_half(0, X, 1, 1)
    for s_ in (2, 3):
        ring_half(0, X, s_, 0)
        ring_half(0, X, s_, 1)
    got("w1", (0,), b.w.at[wrows(1 - X, z), :])
    ring_start(1, 1 - X)
    toky_first()
    m_send()
    ring_half(0, X, 4, 0)
    ring_half(0, X, 4, 1)
    ring_half(1, 1 - X, 1, 0)
    ring_half(1, 1 - X, 1, 1)
    toky_last()
    norm()
    ready = {
        (2, 0): [(0, X, 1), (0, X, 2)],
        (2, 1): [(0, X, 3), (0, X, 4)],
        (3, 0): [(1, 1 - X, 1)],
        (3, 1): [(1, 1 - X, 2)],
    }
    for at, done in ready.items():
        ring_half(1, 1 - X, *at)
        for d in done:
            other_core(*d)
            multiply(*d[1:])
    ring_half(1, 1 - X, 4, 0)
    ring_half(1, 1 - X, 4, 1)
    for s_ in (3, 4):
        other_core(1, 1 - X, s_)
        multiply(1 - X, s_)

    @pl.loop(0, 5)
    def _(n):
        cs = pl.ds(pl.multiple_of(n * 128, 128), 128)
        g = b.acc[:, cs]
        u = b.acc[:, pl.ds(pl.multiple_of(FH + n * 128, 128), 128)]
        hid = (g / (1.0 + jnp.exp(-g)) * u).T.astype(BF16)
        for k in (0, 1):
            b.hs[k, cs, :] = hid[:, k * TB : (k + 1) * TB]

            @pl.when(c == X)
            def _():
                b.h[c * 16 + k * 8 + z, cs, :] = hid[:, k * TB : (k + 1) * TB]

    @pl.when(c != X)
    def _():
        for k in (0, 1):
            send("hx", (k,), b.hs.at[k], b.h.at[(1 - c) * 16 + k * 8 + z], dev(x_=xo, c_=1 - c))

    got("m1", (0,), b.mx.at[1 - X])
    for k in (0, 1):

        @pl.when(c != X)
        def _():
            got("hx", (k,), hchunk(k, z))

        for d in (0, 1):
            send("hr", (d, 0, k), hchunk(k, z), hchunk(k, z), dz[d])
        send("hd", (0, k), hchunk(k, z), hchunk(k, z), dc)

    def hother(k, z_):
        return b.h.at[(1 - c) * 16 + k * 8 + z_]

    def h_take(n):
        s_ = n // 2 + 1
        for k in (0, 1):

            @pl.when(lax.rem(n, 2) == k)
            def _():
                for d in (0, 1):
                    zz = lax.rem(z + (8 - s_ if d == 0 else s_), 8)
                    r = 8 - s_ if d == 0 else s_
                    ch = hchunk(k, zz)

                    def take():
                        got("hr", (d, s_ - 1, k), ch)

                        @pl.when(s_ < (4 if k == d else 3))
                        def _():
                            send("hr", (d, s_, k), ch, ch, dz[d])

                        send("hd", (r, k), ch, ch, dc)

                    if k == d:
                        take()
                    else:
                        pl.when(s_ < 4)(take)

    def level(i):
        k = (i + 1) // 2
        r = lax.rem(i + par, 2) * (8 - 2 * k) + k
        return lax.rem(r, 8), lax.rem(z + r, 8)

    def place(i):
        _, zz = level(i)
        return zz, lax.rem(zz, 2), lax.rem(zz // 2 - y + 4, 4)

    def plus(u, v):
        return (u.astype(F32) + v.astype(F32)).astype(BF16)

    xn_ = (x // 2) * 2 + 1 - xl
    dxn = dev(x_=xn_)

    def part1(units):
        at = []
        for i, k in units:
            zz, e, rel = place(i)
            r, _ = level(i)
            got("hd", (r, k), hother(k, zz))
            at.append((k * 8 + zz, e, rel))
        halves = [jnp.concatenate([b.h[f * 16 + at[0][0]], b.h[f * 16 + at[1][0]]], axis=1) for f in (0, 1)]
        for Xd in (0, 1):
            t = jnp.dot(b.mx[Xd, :, :FH], halves[0], preferred_element_type=F32)
            t += jnp.dot(b.mx[Xd, :, FH:], halves[1], preferred_element_type=F32)
            for j, (i, k) in enumerate(units):
                u = t[:, j * TB : (j + 1) * TB]
                b.q[i, k, Xd] = u[:NY].astype(BF16)

                @pl.when(xl == k)
                def _():
                    b.sx[i, Xd] = u[NY:]

                @pl.when(xl != k)
                def _():
                    b.px[i, Xd] = u[NY:].astype(BF16)

        for (i, k), (_, e, rel) in zip(units, at):

            @pl.when(xl != k)
            def _():
                send("px", (i,), b.px.at[i], b.rx.at[i], dxn)

            @pl.when(rel == 2)
            def _():
                send("qa", (e, k), b.q.at[i, k], (b.qa if k == 0 else b.qb).at[e], dyp if k == 0 else dym)

            if k == 1:

                @pl.when(rel == 1)
                def _():
                    send("qr", (e, 0), b.q.at[i, 1], b.qr.at[e, 1], dyp)

            else:

                @pl.when(rel == 3)
                def _():
                    send("qr", (e, 1), b.q.at[i, 0], b.ql.at[e, 0], dym)

    def part2s(i):
        _, e, rel = place(i)
        got("px", (i,), b.rx.at[i])
        for Xd in (0, 1):
            b.s[i, Xd] = (b.sx[i, Xd] + b.rx[i, Xd].astype(F32)).astype(BF16)

        @pl.when(rel == 2)
        def _():
            send("ya", (e, 0), b.s.at[i, 0], b.ya.at[e], dyp)
            send("ya", (e, 1), b.s.at[i, 1], b.yb.at[e], dym)

        @pl.when(rel == 1)
        def _():
            send("yr", (e, 0), b.s.at[i, 1], b.yr.at[e, 1], dyp)

        @pl.when(rel == 3)
        def _():
            send("yr", (e, 1), b.s.at[i, 0], b.yl.at[e, 0], dym)

    def part2q(i):
        _, e, rel = place(i)

        @pl.when(rel == 1)
        def _():
            got("qa", (e, 0), b.qa.at[e])
            for Xd in (0, 1):
                b.q[i, 0, Xd] = plus(b.q[i, 0, Xd], b.qa[e, Xd])
            send("qr", (e, 0), b.q.at[i, 0], b.qr.at[e, 0], dyp)

        @pl.when(rel == 3)
        def _():
            got("qa", (e, 1), b.qb.at[e])
            for Xd in (0, 1):
                b.q[i, 1, Xd] = plus(b.q[i, 1, Xd], b.qb[e, Xd])
            send("qr", (e, 1), b.q.at[i, 1], b.ql.at[e, 1], dym)

    def part3s(i):
        _, e, rel = place(i)

        @pl.when(rel == 1)
        def _():
            got("ya", (e, 0), b.ya.at[e])
            b.s[i, 0] = plus(b.s[i, 0], b.ya[e])
            send("yr", (e, 0), b.s.at[i, 0], b.yr.at[e, 0], dyp)

        @pl.when(rel == 3)
        def _():
            got("ya", (e, 1), b.yb.at[e])
            b.s[i, 1] = plus(b.s[i, 1], b.yb[e])
            send("yr", (e, 1), b.s.at[i, 1], b.yl.at[e, 1], dym)

    def part4q(i):
        _, e, rel = place(i)

        @pl.when(rel == 0)
        def _():
            got("qr", (e, 0), b.qr.at[e])
            got("qr", (e, 1), b.ql.at[e])

            @pl.loop(0, 4)
            def _(dx):
                at = (lax.rem(dx, 2), dx // 2)
                u = b.q[i, *at].astype(F32) + b.qr[e, *at].astype(F32) + b.ql[e, *at].astype(F32)
                b.tq[e, *at] = u.astype(BF16)

            for to, tx_ in ((dxo, xo), (dxp, xp), (dxm, xm)):
                send("fq", (e,), b.tq.at[e, lax.rem(tx_, 2), tx_ // 2], b.fq.at[x, e], to)
            b.fq[x, e] = b.tq[e, xl, X]

    def part4s(i):
        _, e, rel = place(i)

        @pl.when(rel == 0)
        def _():
            got("yr", (e, 0), b.yr.at[e])
            got("yr", (e, 1), b.yl.at[e])
            for Xd in (0, 1):
                b.us[e, Xd] = (
                    b.s[i, Xd].astype(F32) + b.yr[e, Xd].astype(F32) + b.yl[e, Xd].astype(F32)
                ).astype(BF16)
            send("fs", (e,), b.us.at[e, 1 - X], b.fs.at[X, e], dxo)
            b.fs[X, e] = b.us[e, X]

    def run(part, i, lag):
        pl.when((i >= lag) & (i < 8 + lag))(lambda: part(i - lag))

    part1(((0, 0), (0, 1)))

    @pl.loop(0, 13)
    def _(n):
        @pl.when(n < 8)
        def _():
            h_take(n)

        run(part2s, n, 1)
        run(part2q, n, 2)
        for k in (0, 1):

            @pl.when((lax.rem(n, 2) == k) & (n < 6))
            def _():
                part1(((n - k + 1, k), (n - k + 2, k)))

        @pl.when(n == 7)
        def _():
            part1(((7, 0), (7, 1)))

        run(part3s, n, 3)
        run(part4q, n, 5)
        run(part4s, n, 5)

    out_copy = pltpu.make_async_copy(b.ov, out, loc.at[0])

    def ph_last():
        for e in (0, 1):
            got("fq", (e,), b.fq.at[pl.ds(0, 3), e])
            got("fs", (e,), b.fs.at[0, e])
            for g in (0, 1):
                lanes = pl.ds(e * 256 + g * TB, TB)
                t = b.fq[2 * g, e].astype(F32) + b.fq[2 * g + 1, e].astype(F32)
                u = b.fs[g, e].astype(F32)
                primal = t[:KD]
                b.ov[:, lanes] = primal.astype(BF16)
                sq = 1.0 / (1.0 + jnp.exp(-primal))
                both = t[KD:] * t[KD:] + u * u
                b.cvs[:, lanes] = jnp.sum(sq * (1.0 - sq) * both, axis=0, keepdims=True)

    ph_last()

    for r in range(1, 32):
        send("cv", (0,), b.cvs, b.cvr.at[r], peers[r - 1])
    out_copy.start()
    got("cv", (0,), b.cvr.at[pl.ds(1, 31)])
    total = b.cvs[...]
    for r in range(1, 32):
        total += b.cvr[r]
    b.cvo[...] = total / (PROBES * D)
    curv_copy = pltpu.make_async_copy(b.cvo, curv, loc.at[1])
    curv_copy.start()

    def ph_drain():
        for k in range(3):
            sent("tokx", tx, k)
        sent("toky", b.xg.at[pl.ds(0, 6)])
        sent("w1", b.w.at[pl.ds(0, KD), :])
        sent("m1", b.mx.at[0])
        sent("wr", b.w.at[pl.ds(0, 14 * KD), :])
        sent("wd", b.w.at[pl.ds(0, 16 * KD), :])

        @pl.when(c != X)
        def _():
            sent("hx", b.h.at[pl.ds(0, 2)])

        sent("hr", b.h.at[pl.ds(0, 14)])
        sent("hd", b.h.at[pl.ds(0, 16)])
        sent("px", b.rx)
        sent("qa", b.q.at[pl.ds(0, 2)])
        sent("qr", b.q.at[pl.ds(0, 4)])
        sent("ya", b.rx.at[pl.ds(0, 2)])
        sent("yr", b.rx.at[pl.ds(0, 4)])
        sent("fq", b.q.at[pl.ds(0, 3), 0])
        sent("fs", b.rx.at[0])
        sent("cv", b.cvr.at[pl.ds(1, 31)])
        out_copy.wait()
        curv_copy.wait()

    ph_drain()


def on_device(tokens, norm_gain, gate_weight, up_weight, down_weight, probes):
    vmem = pl.BlockSpec(memory_space=pltpu.VMEM)
    sems = []
    for name, shape in SEMS.items():
        sems += [pltpu.SemaphoreType.DMA((3,) if name == "tokx" else (1,)), pltpu.SemaphoreType.DMA(shape)]
    out, curv = pl.pallas_call(
        kernel,
        out_shape=(jax.ShapeDtypeStruct((KD, 512), BF16), jax.ShapeDtypeStruct((1, 512), F32)),
        in_specs=[vmem] * 6,
        out_specs=(pl.BlockSpec(memory_space=pl.ANY),) * 2,
        scratch_shapes=[pltpu.VMEM(s, t) for s, t in SCRATCH.values()] + sems + [pltpu.SemaphoreType.DMA((5,))],
        compiler_params=pltpu.CompilerParams(
            collective_id=0, has_side_effects=True, vmem_limit_bytes=60 * 1024 * 1024
        ),
        name="mlp_curv",
    )(tokens.T, norm_gain.reshape(28, 128), gate_weight, up_weight, down_weight, probes)
    return out.T, curv.reshape(512)


def solution(mesh):
    return jax.shard_map(
        on_device,
        mesh=mesh,
        in_specs=(
            P("fsdp", "tp"),
            P(),
            P("fsdp", "tp"),
            P("fsdp", "tp"),
            P("fsdp", "tp"),
            P(None, "fsdp", "tp"),
        ),
        out_specs=(P("tp", "fsdp"), P("tp")),
        check_vma=False,
    )
```

```python
import jax
import jax.numpy as jnp
from jax import lax
from jax.experimental import pallas as pl
from jax.experimental.pallas import tpu as pltpu
from jax.sharding import PartitionSpec as P

MESH = pl.DeviceIdType.MESH
F32, BF16 = jnp.float32, jnp.bfloat16
D = 3584
PROBES = 2
EPS = 1e-06
KD = 112
FH = 640
TB = 128
DT = 448
NY = 176
NX = 3 * KD - NY

SCRATCH = dict(
    tv=((DT, TB), BF16),
    gv=((28, 128), BF16),
    xg=((8, 256, DT), BF16),
    xn=((8, 256, DT), BF16),
    g8=((8, DT), F32),
    w=((D, 2 * FH), BF16),
    acc=((256, 2 * FH), F32),
    hs=((2, FH, TB), BF16),
    h=((32, FH, TB), BF16),
    mx=((2, 3 * KD, 2 * FH), BF16),
    px=((8, 2, NX, TB), BF16),
    rx=((8, 2, NX, TB), BF16),
    sx=((8, 2, NX, TB), F32),
    s=((8, 2, NX, TB), BF16),
    ya=((2, NX, TB), BF16),
    yb=((2, NX, TB), BF16),
    yr=((2, 2, NX, TB), BF16),
    yl=((2, 2, NX, TB), BF16),
    us=((2, 2, NX, TB), BF16),
    fs=((2, 2, NX, TB), BF16),
    q=((8, 2, 2, NY, TB), BF16),
    qa=((2, 2, NY, TB), BF16),
    qb=((2, 2, NY, TB), BF16),
    qr=((2, 2, 2, NY, TB), BF16),
    ql=((2, 2, 2, NY, TB), BF16),
    tq=((2, 2, 2, NY, TB), BF16),
    fq=((4, 2, NY, TB), BF16),
    cvs=((1, 512), F32),
    cvr=((32, 1, 512), F32),
)
SEMS = dict(
    tokx=(3,), toky=(2, 2, 2), w1=(1,), m1=(1,), wr=(2, 2, 4, 2), wd=(2, 8), hx=(2,), hr=(2, 4, 2), hd=(8, 2),
    px=(8,), qa=(2, 2), qr=(2, 2), ya=(2, 2), yr=(2, 2), fq=(2,), fs=(2,), cv=(1,),
)


class Refs:
    pass


def kernel(tok_t, gain, wg, wu, dn, pr, out, curv, *scratch):
    b, ss, rs = Refs(), Refs(), Refs()
    names = list(SCRATCH)
    for n, r in zip(names, scratch):
        setattr(b, n, r)
    rest = scratch[len(names):]
    for i, n in enumerate(SEMS):
        setattr(ss, n, rest[2 * i])
        setattr(rs, n, rest[2 * i + 1])
    loc = rest[2 * len(SEMS)]

    fi, ti = lax.axis_index("fsdp"), lax.axis_index("tp")
    X, z, c = fi // 16, lax.rem(fi // 2, 8), lax.rem(fi, 2)
    xl, y = ti // 4, lax.rem(ti, 4)
    x = X * 2 + xl

    def dev(x_=None, y_=None, z_=None, c_=None):
        x_ = x if x_ is None else x_
        y_ = y if y_ is None else y_
        z_ = z if z_ is None else z_
        c_ = c if c_ is None else c_
        return ((x_ // 2) * 16 + z_ * 2 + c_, lax.rem(x_, 2) * 4 + y_)

    xp, xm, xo = lax.rem(x + 1, 4), lax.rem(x + 3, 4), lax.rem(x + 2, 4)
    yp, ym = lax.rem(y + 1, 4), lax.rem(y + 3, 4)
    dxp, dxm, dxo = dev(x_=xp), dev(x_=xm), dev(x_=xo)
    dyp, dym = dev(y_=yp), dev(y_=ym)
    dz = (dev(z_=lax.rem(z + 1, 8)), dev(z_=lax.rem(z + 7, 8)))
    dc = dev(c_=1 - c)

    def copy(name, idx, src, dst, to):
        out_sem = getattr(ss, name).at[idx[0] if name == "tokx" else 0]
        return pltpu.make_async_remote_copy(
            src_ref=src, dst_ref=dst, send_sem=out_sem, recv_sem=getattr(rs, name).at[idx],
            device_id=to, device_id_type=MESH,
        )

    def send(name, idx, src, dst, to):
        copy(name, idx, src, dst, to).start()

    def got(name, idx, ref):
        copy(name, idx, ref, ref, dc).wait_recv()

    def sent(name, ref, idx=0):
        copy(name, (idx,) + (0,) * (len(SEMS[name]) - 1), ref, ref, dc).wait_send()

    def cols(k):
        return pl.ds(pl.multiple_of(k * FH, 128), FH)

    def wrows(X_, z_, c_=None):
        c_ = c if c_ is None else c_
        return pl.ds(pl.multiple_of((X_ * 16 + z_ * 2 + c_) * KD, 16), KD)

    def wchunk(X_, z_, half):
        return b.w.at[wrows(X_, z_), pl.ds(half * FH, FH)]

    def hchunk(X_, z_):
        return b.h.at[c * 16 + X_ * 8 + z_]

    barrier = pltpu.get_barrier_semaphore()
    peers = [(lax.rem(fi + r, 32), ti) for r in range(1, 32)]
    partners = [dxp, dxm, dyp, dym] + peers
    for p in partners:
        pl.semaphore_signal(barrier, inc=1, device_id=p, device_id_type=MESH)

    mine = [
        (tok_t, b.tv),
        (gain, b.gv),
        (wg.at[:, cols(X)], wchunk(X, z, 0)),
        (wu.at[:, cols(X)], wchunk(X, z, 1)),
        (dn, b.mx.at[X, pl.ds(0, KD), :]),
        (pr.at[0], b.mx.at[X, pl.ds(KD, KD), :]),
        (pr.at[1], b.mx.at[X, pl.ds(2 * KD, KD), :]),
    ]
    own = [pltpu.make_async_copy(s_, d_, loc.at[i]) for i, (s_, d_) in enumerate(mine)]
    for o in own:
        o.start()
    pl.semaphore_wait(barrier, len(partners))
    for o in own[2:4]:
        o.wait()

    def ring_start(sub, X_):
        for h in (0, 1):
            for d in (0, 1):
                ch = wchunk(X_, z, h ^ d)
                send("wr", (d, sub, 0, h ^ d), ch, ch, dz[d])
        send("wd", (sub, 0), b.w.at[wrows(X_, z), :], b.w.at[wrows(X_, z), :], dc)

    ring_start(0, X)
    tx = b.xg.at[ti, pl.ds(pl.multiple_of(X * TB, 128), TB), :]
    own[0].wait()
    tx[...] = b.tv[...].T
    for k, to in enumerate((dxp, dxm, dxo)):
        send("tokx", (k,), tx, tx, to)
    for half, src in enumerate((wg, wu)):
        send("w1", (0,), src.at[:, cols(1 - X)], wchunk(X, z, half), dxo)
    own[1].wait()
    for j in range(8):
        at = j * DT
        while at < (j + 1) * DT:
            n = min(128 - at % 128, (j + 1) * DT - at)
            row, lane = at // 128, at % 128
            b.g8[j : j + 1, at - j * DT : at - j * DT + n] = b.gv[row : row + 1, lane : lane + n].astype(F32)
            at += n
    for o in own[4:]:
        o.wait()

    def m_send():
        send("m1", (0,), b.mx.at[X], b.mx.at[X], dxo)

    def zsrc(d, s_):
        return lax.rem(z + (8 - s_ if d == 0 else s_), 8)

    def ring_half(sub, X_, s_, h):
        for d in (0, 1):
            ch = wchunk(X_, zsrc(d, s_), h ^ d)
            got("wr", (d, sub, s_ - 1, h ^ d), ch)
            if s_ < 3 or (s_ == 3 and h == 0):
                send("wr", (d, sub, s_, h ^ d), ch, ch, dz[d])
        if h == 1 or s_ == 4:
            for d in (0, 1):
                if s_ == 4 and d == 1:
                    continue
                blk = b.w.at[wrows(X_, zsrc(d, s_)), :]
                send("wd", (sub, 8 - s_ if d == 0 else s_), blk, blk, dc)

    par = lax.rem(z, 2)

    def pair(i):
        f = 3 * i - 5 * (i // 2) - 2 * (i // 3)
        return lax.rem(z // 2 + f * (1 - par) + (4 - f) * par, 4)

    def other_core(sub, X_, s_):
        if s_ == 1:
            got("wd", (sub, 0), b.w.at[wrows(X_, z, 1 - c), :])
        for d in (0, 1):
            if s_ == 4 and d == 1:
                continue
            got("wd", (sub, 8 - s_ if d == 0 else s_), b.w.at[wrows(X_, zsrc(d, s_), 1 - c), :])

    def multiply(X_, s_):
        j = X_ * 4 + pair(s_ - 1)

        @pl.loop(0, 5)
        def _(n):
            cs = pl.ds(pl.multiple_of(n * 256, 256), 256)
            ks = pl.ds(pl.multiple_of(j * DT, 64), DT)
            b.acc[:, cs] += jnp.dot(b.xn[j], b.w[ks, cs], preferred_element_type=F32)

    def tokx_done():
        for k, sx in enumerate((xm, xp, xo)):
            got("tokx", (k,), b.xg.at[lax.rem(sx, 2) * 4 + y, pl.ds(pl.multiple_of((sx // 2) * TB, 128), TB), :])
        for k in (0, 1):
            blk = b.xg.at[k * 4 + y]
            send("toky", (0, k, 0), blk, blk, dyp)
            send("toky", (1, k, 0), blk, blk, dym)

    def toky_first():
        for d, sy, to in ((0, ym, dyp), (1, yp, dym)):
            for k in (0, 1):
                got("toky", (d, k, 0), b.xg.at[k * 4 + sy])
            blk = b.xg.at[d * 4 + sy]
            send("toky", (d, d, 1), blk, blk, to)

    def toky_last():
        for d in (0, 1):
            got("toky", (d, d, 1), b.xg.at[d * 4 + lax.rem(y + 2, 4)])

    def norm():
        @pl.loop(0, 8)
        def _(t):
            rows = pl.ds(pl.multiple_of(t * 32, 32), 32)
            total = jnp.zeros((32, 1), F32)
            for j in range(8):
                v = b.xg[j, rows, :].astype(F32)
                total += jnp.sum(v * v, axis=1, keepdims=True)
            inv = lax.rsqrt(total / D + EPS)
            for j in range(8):
                v = b.xg[j, rows, :].astype(F32)
                b.xn[j, rows, :] = (v * inv * b.g8[j : j + 1, :]).astype(BF16)

    b.acc[...] = jnp.zeros_like(b.acc)
    ring_half(0, X, 1, 0)
    tokx_done()
    ring_half(0, X, 1, 1)
    ring_half(0, X, 2, 0)
    ring_half(0, X, 2, 1)
    ring_half(0, X, 3, 0)
    got("w1", (0,), b.w.at[wrows(1 - X, z), :])
    ring_start(1, 1 - X)
    ring_half(0, X, 3, 1)
    toky_first()
    m_send()
    ring_half(0, X, 4, 0)
    ring_half(1, 1 - X, 1, 0)
    ring_half(1, 1 - X, 1, 1)
    toky_last()
    norm()
    ready = {
        (2, 0): [(0, X, 1), (0, X, 2)],
        (2, 1): [(0, X, 3), (0, X, 4)],
        (3, 0): [(1, 1 - X, 1)],
        (3, 1): [(1, 1 - X, 2)],
    }
    for at, done in ready.items():
        ring_half(1, 1 - X, *at)
        for d in done:
            other_core(*d)
            multiply(*d[1:])
    ring_half(1, 1 - X, 4, 0)
    for s_ in (3, 4):
        other_core(1, 1 - X, s_)
        multiply(1 - X, s_)

    @pl.loop(0, 5)
    def _(n):
        cs = pl.ds(pl.multiple_of(n * 128, 128), 128)
        g = b.acc[:, cs]
        u = b.acc[:, pl.ds(pl.multiple_of(FH + n * 128, 128), 128)]
        hid = (g / (1.0 + jnp.exp(-g)) * u).T.astype(BF16)
        for k in (0, 1):
            b.hs[k, cs, :] = hid[:, k * TB : (k + 1) * TB]

            @pl.when(c == X)
            def _():
                b.h[c * 16 + k * 8 + z, cs, :] = hid[:, k * TB : (k + 1) * TB]

    @pl.when(c != X)
    def _():
        for k in (0, 1):
            send("hx", (k,), b.hs.at[k], b.h.at[(1 - c) * 16 + k * 8 + z], dev(x_=xo, c_=1 - c))

    got("m1", (0,), b.mx.at[1 - X])
    for k, ways in ((0, ((0, 0),)), (1, ((1, 1), (0, 1), (1, 0)))):

        @pl.when(c != X)
        def _():
            got("hx", (k,), hchunk(k, z))

        for d, kk in ways:
            send("hr", (d, 0, kk), hchunk(kk, z), hchunk(kk, z), dz[d])
        send("hd", (0, k), hchunk(k, z), hchunk(k, z), dc)

    def hother(k, z_):
        return b.h.at[(1 - c) * 16 + k * 8 + z_]

    def h_take(n):
        s_ = n // 2 + 1
        for h in (0, 1):

            @pl.when(lax.rem(n, 2) == h)
            def _():
                for d in (0, 1):
                    k = h ^ d
                    ch = hchunk(k, lax.rem(z + (8 - s_ if d == 0 else s_), 8))
                    got("hr", (d, s_ - 1, k), ch)

                    @pl.when(s_ < 4 - h)
                    def _():
                        send("hr", (d, s_, k), ch, ch, dz[d])

                    send("hd", (8 - s_ if d == 0 else s_, k), ch, ch, dc)

    def level(i):
        k = (i + 1) // 2
        r = lax.rem(i + par, 2) * (8 - 2 * k) + k
        return lax.rem(r, 8), lax.rem(z + r, 8)

    def place(i):
        _, zz = level(i)
        return zz, lax.rem(zz, 2), lax.rem(zz // 2 - y + 4, 4)

    def plus(u, v):
        return (u.astype(F32) + v.astype(F32)).astype(BF16)

    xn_ = (x // 2) * 2 + 1 - xl
    dxn = dev(x_=xn_)

    def part1(units):
        at = []
        for i, k in units:
            zz, e, rel = place(i)
            r, _ = level(i)
            got("hd", (r, k), hother(k, zz))
            at.append((k * 8 + zz, e, rel))
        halves = [jnp.concatenate([b.h[f * 16 + at[0][0]], b.h[f * 16 + at[1][0]]], axis=1) for f in (0, 1)]
        for Xd in (0, 1):
            t = jnp.dot(b.mx[Xd, :, :FH], halves[0], preferred_element_type=F32)
            t += jnp.dot(b.mx[Xd, :, FH:], halves[1], preferred_element_type=F32)
            for j, (i, k) in enumerate(units):
                u = t[:, j * TB : (j + 1) * TB]
                b.q[i, k, Xd] = u[:NY].astype(BF16)

                @pl.when(xl == k)
                def _():
                    b.sx[i, Xd] = u[NY:]

                @pl.when(xl != k)
                def _():
                    b.px[i, Xd] = u[NY:].astype(BF16)

        for (i, k), (_, e, rel) in zip(units, at):

            @pl.when(xl != k)
            def _():
                send("px", (i,), b.px.at[i], b.rx.at[i], dxn)

            @pl.when(rel == 2)
            def _():
                send("qa", (e, k), b.q.at[i, k], (b.qa if k == 0 else b.qb).at[e], dyp if k == 0 else dym)

            if k == 1:

                @pl.when(rel == 1)
                def _():
                    send("qr", (e, 0), b.q.at[i, 1], b.qr.at[e, 1], dyp)

            else:

                @pl.when(rel == 3)
                def _():
                    send("qr", (e, 1), b.q.at[i, 0], b.ql.at[e, 0], dym)

    def part2s(i):
        _, e, rel = place(i)
        got("px", (i,), b.rx.at[i])
        for Xd in (0, 1):
            b.s[i, Xd] = (b.sx[i, Xd] + b.rx[i, Xd].astype(F32)).astype(BF16)

        @pl.when(rel == 2)
        def _():
            send("ya", (e, 0), b.s.at[i, 0], b.ya.at[e], dyp)
            send("ya", (e, 1), b.s.at[i, 1], b.yb.at[e], dym)

        @pl.when(rel == 1)
        def _():
            send("yr", (e, 0), b.s.at[i, 1], b.yr.at[e, 1], dyp)

        @pl.when(rel == 3)
        def _():
            send("yr", (e, 1), b.s.at[i, 0], b.yl.at[e, 0], dym)

    def part2q(i):
        _, e, rel = place(i)

        @pl.when(rel == 1)
        def _():
            got("qa", (e, 0), b.qa.at[e])
            for Xd in (0, 1):
                b.q[i, 0, Xd] = plus(b.q[i, 0, Xd], b.qa[e, Xd])
            send("qr", (e, 0), b.q.at[i, 0], b.qr.at[e, 0], dyp)

        @pl.when(rel == 3)
        def _():
            got("qa", (e, 1), b.qb.at[e])
            for Xd in (0, 1):
                b.q[i, 1, Xd] = plus(b.q[i, 1, Xd], b.qb[e, Xd])
            send("qr", (e, 1), b.q.at[i, 1], b.ql.at[e, 1], dym)

    def part3s(i):
        _, e, rel = place(i)

        @pl.when(rel == 1)
        def _():
            got("ya", (e, 0), b.ya.at[e])
            b.s[i, 0] = plus(b.s[i, 0], b.ya[e])
            send("yr", (e, 0), b.s.at[i, 0], b.yr.at[e, 0], dyp)

        @pl.when(rel == 3)
        def _():
            got("ya", (e, 1), b.yb.at[e])
            b.s[i, 1] = plus(b.s[i, 1], b.yb[e])
            send("yr", (e, 1), b.s.at[i, 1], b.yl.at[e, 1], dym)

    def part4q(i):
        _, e, rel = place(i)

        @pl.when(rel == 0)
        def _():
            got("qr", (e, 0), b.qr.at[e])
            got("qr", (e, 1), b.ql.at[e])

            @pl.loop(0, 4)
            def _(dx):
                at = (lax.rem(dx, 2), dx // 2)
                u = b.q[i, *at].astype(F32) + b.qr[e, *at].astype(F32) + b.ql[e, *at].astype(F32)
                b.tq[e, *at] = u.astype(BF16)

            for to, tx_ in ((dxo, xo), (dxp, xp), (dxm, xm)):
                send("fq", (e,), b.tq.at[e, lax.rem(tx_, 2), tx_ // 2], b.fq.at[x, e], to)
            b.fq[x, e] = b.tq[e, xl, X]

    def part4s(i):
        _, e, rel = place(i)

        @pl.when(rel == 0)
        def _():
            got("yr", (e, 0), b.yr.at[e])
            got("yr", (e, 1), b.yl.at[e])
            for Xd in (0, 1):
                b.us[e, Xd] = (
                    b.s[i, Xd].astype(F32) + b.yr[e, Xd].astype(F32) + b.yl[e, Xd].astype(F32)
                ).astype(BF16)
            send("fs", (e,), b.us.at[e, 1 - X], b.fs.at[X, e], dxo)
            b.fs[X, e] = b.us[e, X]

    def run(part, i, lag):
        pl.when((i >= lag) & (i < 8 + lag))(lambda: part(i - lag))

    ahead = 1 - lax.rem(c + X, 2)
    h_take(0)
    pl.when(ahead == 1)(lambda: h_take(1))
    part1(((0, 0), (0, 1)))
    pl.when(ahead == 0)(lambda: h_take(1))

    @pl.loop(0, 14)
    def _(n):
        nn = n + 2 * ahead

        @pl.when((nn >= 2) & (nn < 7))
        def _():
            h_take(nn)

        run(part2s, n, 2)
        run(part2q, n, 2)
        for h in (0, 1):

            @pl.when((lax.rem(n, 2) == h) & (n < 6))
            def _():
                part1(((n - h + 1 + par, h), (n - h + 2 - par, 1 - h)))

        @pl.when(n == 6)
        def _():
            part1(((7, 0), (7, 1)))

        run(part3s, n, 5)
        run(part4q, n, 6)
        run(part4s, n, 6)

    def ph_last():
        for e in (0, 1):
            got("fq", (e,), b.fq.at[pl.ds(0, 3), e])
            got("fs", (e,), b.fs.at[0, e])
            for g in (0, 1):
                lanes = pl.ds(e * 256 + g * TB, TB)
                t = b.fq[2 * g, e].astype(F32) + b.fq[2 * g + 1, e].astype(F32)
                u = b.fs[g, e].astype(F32)
                primal = t[:KD]
                out[:, lanes] = primal.astype(BF16)
                sq = 1.0 / (1.0 + jnp.exp(-primal))
                slope = sq * (1.0 - sq)
                first, rest = NY - KD, 2 * KD - NY
                total = jnp.sum(slope[:first] * t[KD:] * t[KD:], axis=0, keepdims=True)
                total += jnp.sum(slope[first:] * u[:rest] * u[:rest], axis=0, keepdims=True)
                total += jnp.sum(slope * u[rest:] * u[rest:], axis=0, keepdims=True)
                b.cvs[:, lanes] = total

    ph_last()

    for r in range(1, 32):
        send("cv", (0,), b.cvs, b.cvr.at[r], peers[r - 1])
    got("cv", (0,), b.cvr.at[pl.ds(1, 31)])
    total = b.cvs[...]
    for r in range(1, 32):
        total += b.cvr[r]
    curv[...] = total / (PROBES * D)

    def ph_drain():
        for k in range(3):
            sent("tokx", tx, k)
        sent("toky", b.xg.at[pl.ds(0, 6)])
        sent("w1", b.w.at[pl.ds(0, KD), :])
        sent("m1", b.mx.at[0])
        sent("wr", b.w.at[pl.ds(0, 14 * KD), :])
        sent("wd", b.w.at[pl.ds(0, 16 * KD), :])

        @pl.when(c != X)
        def _():
            sent("hx", b.h.at[pl.ds(0, 2)])

        sent("hr", b.h.at[pl.ds(0, 14)])
        sent("hd", b.h.at[pl.ds(0, 16)])
        sent("px", b.rx)
        sent("qa", b.q.at[pl.ds(0, 2)])
        sent("qr", b.q.at[pl.ds(0, 4)])
        sent("ya", b.rx.at[pl.ds(0, 2)])
        sent("yr", b.rx.at[pl.ds(0, 4)])
        sent("fq", b.q.at[pl.ds(0, 3), 0])
        sent("fs", b.rx.at[0])
        sent("cv", b.cvr.at[pl.ds(1, 31)])

    ph_drain()


def on_device(tokens, norm_gain, gate_weight, up_weight, down_weight, probes):
    vmem = pl.BlockSpec(memory_space=pltpu.VMEM)
    hbm = pl.BlockSpec(memory_space=pl.ANY)
    sems = []
    for name, shape in SEMS.items():
        sems += [pltpu.SemaphoreType.DMA((3,) if name == "tokx" else (1,)), pltpu.SemaphoreType.DMA(shape)]
    out, curv = pl.pallas_call(
        kernel,
        out_shape=(pltpu.VMEM((KD, 512), BF16), pltpu.VMEM((1, 512), F32)),
        in_specs=[hbm] * 6,
        out_specs=(vmem, vmem),
        scratch_shapes=[pltpu.VMEM(s, t) for s, t in SCRATCH.values()] + sems + [pltpu.SemaphoreType.DMA((7,))],
        compiler_params=pltpu.CompilerParams(
            collective_id=0, has_side_effects=True, vmem_limit_bytes=60 * 1024 * 1024
        ),
        name="mlp_curv",
    )(tokens.T, norm_gain.reshape(28, 128), gate_weight, up_weight, down_weight, probes)
    return out.T, curv.reshape(512)


def solution(mesh):
    return jax.shard_map(
        on_device,
        mesh=mesh,
        in_specs=(
            P("fsdp", "tp"),
            P(),
            P("fsdp", "tp"),
            P("fsdp", "tp"),
            P("fsdp", "tp"),
            P(None, "fsdp", "tp"),
        ),
        out_specs=(P("tp", "fsdp"), P("tp")),
        check_vma=False,
    )
```

```python
import jax
import jax.numpy as jnp
from jax import lax
from jax.experimental import pallas as pl
from jax.experimental.pallas import tpu as pltpu
from jax.sharding import PartitionSpec as P

MESH = pl.DeviceIdType.MESH
F32, BF16 = jnp.float32, jnp.bfloat16
D = 3584
PROBES = 2
EPS = 1e-06
KD = 112
FH = 640
TB = 128
DT = 448
NY = 144
NX = 3 * KD - NY

SCRATCH = dict(
    tv=((DT, TB), BF16),
    gv=((28, 128), BF16),
    xg=((8, 256, DT), BF16),
    xn=((8, 256, DT), BF16),
    g8=((8, DT), F32),
    w=((D, 2 * FH), BF16),
    acc=((256, 2 * FH), F32),
    hs=((2, FH, TB), BF16),
    h=((32, FH, TB), BF16),
    mx=((2, 3 * KD, 2 * FH), BF16),
    px=((8, 2, NX, TB), BF16),
    rx=((8, 2, NX, TB), BF16),
    sx=((8, 2, NX, TB), F32),
    s=((8, 2, NX, TB), BF16),
    ya=((2, NX, TB), BF16),
    yb=((2, NX, TB), BF16),
    yr=((2, 2, NX, TB), BF16),
    yl=((2, 2, NX, TB), BF16),
    us=((2, 2, NX, TB), BF16),
    fs=((2, 2, NX, TB), BF16),
    q=((8, 2, 2, NY, TB), BF16),
    qa=((2, 2, NY, TB), BF16),
    qb=((2, 2, NY, TB), BF16),
    qr=((2, 2, 2, NY, TB), BF16),
    ql=((2, 2, 2, NY, TB), BF16),
    tq=((2, 2, 2, NY, TB), BF16),
    fq=((4, 2, NY, TB), BF16),
    cvs=((1, 512), F32),
    cvr=((32, 1, 512), F32),
)
SEMS = dict(
    tokx=(3,), toky=(2, 2, 2), w1=(1,), m1=(1,), wr=(2, 2, 4, 2), wd=(2, 8), hx=(2,), hr=(2, 4, 2), hd=(8, 2),
    px=(8,), qa=(2, 2), qr=(2, 2), ya=(2, 2), yr=(2, 2), fq=(2,), fs=(2,), cv=(1,),
)


class Refs:
    pass


def kernel(tok_t, gain, wg, wu, dn, pr, out, curv, *scratch):
    b, ss, rs = Refs(), Refs(), Refs()
    names = list(SCRATCH)
    for n, r in zip(names, scratch):
        setattr(b, n, r)
    rest = scratch[len(names):]
    for i, n in enumerate(SEMS):
        setattr(ss, n, rest[2 * i])
        setattr(rs, n, rest[2 * i + 1])
    loc = rest[2 * len(SEMS)]

    fi, ti = lax.axis_index("fsdp"), lax.axis_index("tp")
    X, z, c = fi // 16, lax.rem(fi // 2, 8), lax.rem(fi, 2)
    xl, y = ti // 4, lax.rem(ti, 4)
    x = X * 2 + xl

    def dev(x_=None, y_=None, z_=None, c_=None):
        x_ = x if x_ is None else x_
        y_ = y if y_ is None else y_
        z_ = z if z_ is None else z_
        c_ = c if c_ is None else c_
        return ((x_ // 2) * 16 + z_ * 2 + c_, lax.rem(x_, 2) * 4 + y_)

    xp, xm, xo = lax.rem(x + 1, 4), lax.rem(x + 3, 4), lax.rem(x + 2, 4)
    yp, ym = lax.rem(y + 1, 4), lax.rem(y + 3, 4)
    dxp, dxm, dxo = dev(x_=xp), dev(x_=xm), dev(x_=xo)
    dyp, dym = dev(y_=yp), dev(y_=ym)
    dz = (dev(z_=lax.rem(z + 1, 8)), dev(z_=lax.rem(z + 7, 8)))
    dc = dev(c_=1 - c)

    def copy(name, idx, src, dst, to):
        out_sem = getattr(ss, name).at[idx[0] if name == "tokx" else 0]
        return pltpu.make_async_remote_copy(
            src_ref=src, dst_ref=dst, send_sem=out_sem, recv_sem=getattr(rs, name).at[idx],
            device_id=to, device_id_type=MESH,
        )

    def send(name, idx, src, dst, to):
        copy(name, idx, src, dst, to).start()

    def got(name, idx, ref):
        copy(name, idx, ref, ref, dc).wait_recv()

    def sent(name, ref, idx=0):
        copy(name, (idx,) + (0,) * (len(SEMS[name]) - 1), ref, ref, dc).wait_send()

    def cols(k):
        return pl.ds(pl.multiple_of(k * FH, 128), FH)

    def wrows(X_, z_, c_=None):
        c_ = c if c_ is None else c_
        return pl.ds(pl.multiple_of((X_ * 16 + z_ * 2 + c_) * KD, 16), KD)

    def wchunk(X_, z_, half):
        return b.w.at[wrows(X_, z_), pl.ds(half * FH, FH)]

    def hchunk(X_, z_):
        return b.h.at[c * 16 + X_ * 8 + z_]

    barrier = pltpu.get_barrier_semaphore()
    peers = [(lax.rem(fi + r, 32), ti) for r in range(1, 32)]
    partners = [dxp, dxm, dyp, dym] + peers
    for p in partners:
        pl.semaphore_signal(barrier, inc=1, device_id=p, device_id_type=MESH)

    mine = [
        (tok_t, b.tv),
        (gain, b.gv),
        (wg.at[:, cols(X)], wchunk(X, z, 0)),
        (wu.at[:, cols(X)], wchunk(X, z, 1)),
        (dn, b.mx.at[X, pl.ds(0, KD), :]),
        (pr.at[0], b.mx.at[X, pl.ds(KD, KD), :]),
        (pr.at[1], b.mx.at[X, pl.ds(2 * KD, KD), :]),
    ]
    own = [pltpu.make_async_copy(s_, d_, loc.at[i]) for i, (s_, d_) in enumerate(mine)]
    for o in own:
        o.start()
    pl.semaphore_wait(barrier, len(partners))
    for o in own[2:4]:
        o.wait()

    def ring_start(sub, X_):
        for h in (0, 1):
            for d in (0, 1):
                ch = wchunk(X_, z, h ^ d)
                send("wr", (d, sub, 0, h ^ d), ch, ch, dz[d])
        send("wd", (sub, 0), b.w.at[wrows(X_, z), :], b.w.at[wrows(X_, z), :], dc)

    ring_start(0, X)
    tx = b.xg.at[ti, pl.ds(pl.multiple_of(X * TB, 128), TB), :]
    own[0].wait()
    tx[...] = b.tv[...].T
    for k, to in enumerate((dxp, dxm, dxo)):
        send("tokx", (k,), tx, tx, to)
    for half, src in enumerate((wg, wu)):
        send("w1", (0,), src.at[:, cols(1 - X)], wchunk(X, z, half), dxo)
    own[1].wait()
    for j in range(8):
        at = j * DT
        while at < (j + 1) * DT:
            n = min(128 - at % 128, (j + 1) * DT - at)
            row, lane = at // 128, at % 128
            b.g8[j : j + 1, at - j * DT : at - j * DT + n] = b.gv[row : row + 1, lane : lane + n].astype(F32)
            at += n
    for o in own[4:]:
        o.wait()

    def m_send():
        send("m1", (0,), b.mx.at[X], b.mx.at[X], dxo)

    def zsrc(d, s_):
        return lax.rem(z + (8 - s_ if d == 0 else s_), 8)

    def ring_half(sub, X_, s_, h):
        for d in (0, 1):
            ch = wchunk(X_, zsrc(d, s_), h ^ d)
            got("wr", (d, sub, s_ - 1, h ^ d), ch)
            if s_ < 3 or (s_ == 3 and h == 0):
                send("wr", (d, sub, s_, h ^ d), ch, ch, dz[d])
        if h == 1 or s_ == 4:
            for d in (0, 1):
                if s_ == 4 and d == 1:
                    continue
                blk = b.w.at[wrows(X_, zsrc(d, s_)), :]
                send("wd", (sub, 8 - s_ if d == 0 else s_), blk, blk, dc)

    par = lax.rem(z, 2)

    def pair(i):
        f = 3 * i - 5 * (i // 2) - 2 * (i // 3)
        return lax.rem(z // 2 + f * (1 - par) + (4 - f) * par, 4)

    def other_core(sub, X_, s_):
        if s_ == 1:
            got("wd", (sub, 0), b.w.at[wrows(X_, z, 1 - c), :])
        for d in (0, 1):
            if s_ == 4 and d == 1:
                continue
            got("wd", (sub, 8 - s_ if d == 0 else s_), b.w.at[wrows(X_, zsrc(d, s_), 1 - c), :])

    def multiply(X_, s_):
        j = X_ * 4 + pair(s_ - 1)

        @pl.loop(0, 5)
        def _(n):
            cs = pl.ds(pl.multiple_of(n * 256, 256), 256)
            ks = pl.ds(pl.multiple_of(j * DT, 64), DT)
            b.acc[:, cs] += jnp.dot(b.xn[j], b.w[ks, cs], preferred_element_type=F32)

    def tokx_done():
        for k, sx in enumerate((xm, xp, xo)):
            got("tokx", (k,), b.xg.at[lax.rem(sx, 2) * 4 + y, pl.ds(pl.multiple_of((sx // 2) * TB, 128), TB), :])
        for k in (0, 1):
            blk = b.xg.at[k * 4 + y]
            send("toky", (0, k, 0), blk, blk, dyp)
            send("toky", (1, k, 0), blk, blk, dym)

    def toky_first():
        for d, sy, to in ((0, ym, dyp), (1, yp, dym)):
            for k in (0, 1):
                got("toky", (d, k, 0), b.xg.at[k * 4 + sy])
            blk = b.xg.at[d * 4 + sy]
            send("toky", (d, d, 1), blk, blk, to)

    def toky_last():
        for d in (0, 1):
            got("toky", (d, d, 1), b.xg.at[d * 4 + lax.rem(y + 2, 4)])

    def norm():
        @pl.loop(0, 8)
        def _(t):
            rows = pl.ds(pl.multiple_of(t * 32, 32), 32)
            total = jnp.zeros((32, 1), F32)
            for j in range(8):
                v = b.xg[j, rows, :].astype(F32)
                total += jnp.sum(v * v, axis=1, keepdims=True)
            inv = lax.rsqrt(total / D + EPS)
            for j in range(8):
                v = b.xg[j, rows, :].astype(F32)
                b.xn[j, rows, :] = (v * inv * b.g8[j : j + 1, :]).astype(BF16)

    b.acc[...] = jnp.zeros_like(b.acc)
    ring_half(0, X, 1, 0)
    tokx_done()
    ring_half(0, X, 1, 1)
    ring_half(0, X, 2, 0)
    ring_half(0, X, 2, 1)
    ring_half(0, X, 3, 0)
    got("w1", (0,), b.w.at[wrows(1 - X, z), :])
    ring_start(1, 1 - X)
    ring_half(0, X, 3, 1)
    toky_first()
    m_send()
    ring_half(0, X, 4, 0)
    ring_half(1, 1 - X, 1, 0)
    ring_half(1, 1 - X, 1, 1)
    toky_last()
    norm()
    ready = {
        (2, 0): [(0, X, 1), (0, X, 2)],
        (2, 1): [(0, X, 3), (0, X, 4)],
        (3, 0): [(1, 1 - X, 1)],
        (3, 1): [(1, 1 - X, 2)],
    }
    for at, done in ready.items():
        ring_half(1, 1 - X, *at)
        for d in done:
            other_core(*d)
            multiply(*d[1:])
    ring_half(1, 1 - X, 4, 0)
    other_core(1, 1 - X, 3)
    multiply(1 - X, 3)
    other_core(1, 1 - X, 4)

    def swap(k, rows):
        src, dst = b.hs.at[k, rows], b.h.at[(1 - c) * 16 + k * 8 + z, rows]
        pl.when(c != X)(lambda: send("hx", (k,), src, dst, dev(x_=xo, c_=1 - c)))

    j = (1 - X) * 4 + pair(3)
    ks = pl.ds(pl.multiple_of(j * DT, 64), DT)
    for n in range(5):
        cs, us = pl.ds(n * 128, 128), pl.ds(FH + n * 128, 128)
        both = jnp.concatenate([b.w[ks, cs], b.w[ks, us]], axis=1)
        t = jnp.dot(b.xn[j], both, preferred_element_type=F32)
        g, u = b.acc[:, cs] + t[:, :128], b.acc[:, us] + t[:, 128:]
        hid = (g / (1.0 + jnp.exp(-g)) * u).T.astype(BF16)
        for k in (0, 1):
            part = hid[:, k * TB : (k + 1) * TB]
            b.hs[k, cs, :] = part

            @pl.when(c == X)
            def _():
                b.h[c * 16 + k * 8 + z, cs, :] = part

        if n:
            swap(0, pl.ds((n - 1) * 128, 128))
    swap(0, pl.ds(512, 128))
    swap(1, pl.ds(0, FH))

    got("m1", (0,), b.mx.at[1 - X])
    for k, ways in ((0, ((0, 0),)), (1, ((1, 1), (0, 1), (1, 0)))):

        @pl.when(c != X)
        def _():
            got("hx", (k,), hchunk(k, z))

        for d, kk in ways:
            send("hr", (d, 0, kk), hchunk(kk, z), hchunk(kk, z), dz[d])
        send("hd", (0, k), hchunk(k, z), hchunk(k, z), dc)

    def hother(k, z_):
        return b.h.at[(1 - c) * 16 + k * 8 + z_]

    def h_take(n):
        s_ = n // 2 + 1
        for h in (0, 1):

            @pl.when(lax.rem(n, 2) == h)
            def _():
                for d in (0, 1):
                    k = h ^ d
                    ch = hchunk(k, lax.rem(z + (8 - s_ if d == 0 else s_), 8))
                    got("hr", (d, s_ - 1, k), ch)

                    @pl.when(s_ < 4 - h)
                    def _():
                        send("hr", (d, s_, k), ch, ch, dz[d])

                    send("hd", (8 - s_ if d == 0 else s_, k), ch, ch, dc)

    def level(i):
        k = (i + 1) // 2
        r = lax.rem(i + par, 2) * (8 - 2 * k) + k
        return lax.rem(r, 8), lax.rem(z + r, 8)

    def place(i):
        _, zz = level(i)
        return zz, lax.rem(zz, 2), lax.rem(zz // 2 - y + 4, 4)

    def plus(u, v):
        return (u.astype(F32) + v.astype(F32)).astype(BF16)

    xn_ = (x // 2) * 2 + 1 - xl
    dxn = dev(x_=xn_)

    def part1(units):
        at = []
        for i, k in units:
            zz, e, rel = place(i)
            r, _ = level(i)
            got("hd", (r, k), hother(k, zz))
            at.append((k * 8 + zz, e, rel))
        halves = [jnp.concatenate([b.h[f * 16 + at[0][0]], b.h[f * 16 + at[1][0]]], axis=1) for f in (0, 1)]
        for Xd in (0, 1):
            t = jnp.dot(b.mx[Xd, :, :FH], halves[0], preferred_element_type=F32)
            t += jnp.dot(b.mx[Xd, :, FH:], halves[1], preferred_element_type=F32)
            for j, (i, k) in enumerate(units):
                u = t[:, j * TB : (j + 1) * TB]
                b.q[i, k, Xd] = u[:NY].astype(BF16)

                @pl.when(xl == k)
                def _():
                    b.sx[i, Xd] = u[NY:]

                @pl.when(xl != k)
                def _():
                    b.px[i, Xd] = u[NY:].astype(BF16)

        for (i, k), (_, e, rel) in zip(units, at):

            @pl.when(xl != k)
            def _():
                send("px", (i,), b.px.at[i], b.rx.at[i], dxn)

            @pl.when(rel == 2)
            def _():
                send("qa", (e, k), b.q.at[i, k], (b.qa if k == 0 else b.qb).at[e], dyp if k == 0 else dym)

            if k == 1:

                @pl.when(rel == 1)
                def _():
                    send("qr", (e, 0), b.q.at[i, 1], b.qr.at[e, 1], dyp)

            else:

                @pl.when(rel == 3)
                def _():
                    send("qr", (e, 1), b.q.at[i, 0], b.ql.at[e, 0], dym)

    def part2s(i):
        _, e, rel = place(i)
        got("px", (i,), b.rx.at[i])
        for Xd in (0, 1):
            b.s[i, Xd] = (b.sx[i, Xd] + b.rx[i, Xd].astype(F32)).astype(BF16)

        @pl.when(rel == 2)
        def _():
            send("ya", (e, 0), b.s.at[i, 0], b.ya.at[e], dyp)
            send("ya", (e, 1), b.s.at[i, 1], b.yb.at[e], dym)

        @pl.when(rel == 1)
        def _():
            send("yr", (e, 0), b.s.at[i, 1], b.yr.at[e, 1], dyp)

        @pl.when(rel == 3)
        def _():
            send("yr", (e, 1), b.s.at[i, 0], b.yl.at[e, 0], dym)

    def part2q(i):
        _, e, rel = place(i)

        @pl.when(rel == 1)
        def _():
            got("qa", (e, 0), b.qa.at[e])
            for Xd in (0, 1):
                b.q[i, 0, Xd] = plus(b.q[i, 0, Xd], b.qa[e, Xd])
            send("qr", (e, 0), b.q.at[i, 0], b.qr.at[e, 0], dyp)

        @pl.when(rel == 3)
        def _():
            got("qa", (e, 1), b.qb.at[e])
            for Xd in (0, 1):
                b.q[i, 1, Xd] = plus(b.q[i, 1, Xd], b.qb[e, Xd])
            send("qr", (e, 1), b.q.at[i, 1], b.ql.at[e, 1], dym)

    def part3s(i):
        _, e, rel = place(i)

        @pl.when(rel == 1)
        def _():
            got("ya", (e, 0), b.ya.at[e])
            b.s[i, 0] = plus(b.s[i, 0], b.ya[e])
            send("yr", (e, 0), b.s.at[i, 0], b.yr.at[e, 0], dyp)

        @pl.when(rel == 3)
        def _():
            got("ya", (e, 1), b.yb.at[e])
            b.s[i, 1] = plus(b.s[i, 1], b.yb[e])
            send("yr", (e, 1), b.s.at[i, 1], b.yl.at[e, 1], dym)

    def part4q(i):
        _, e, rel = place(i)

        @pl.when(rel == 0)
        def _():
            got("qr", (e, 0), b.qr.at[e])
            got("qr", (e, 1), b.ql.at[e])

            @pl.loop(0, 4)
            def _(dx):
                at = (lax.rem(dx, 2), dx // 2)
                u = b.q[i, *at].astype(F32) + b.qr[e, *at].astype(F32) + b.ql[e, *at].astype(F32)
                b.tq[e, *at] = u.astype(BF16)

            for to, tx_ in ((dxo, xo), (dxp, xp), (dxm, xm)):
                send("fq", (e,), b.tq.at[e, lax.rem(tx_, 2), tx_ // 2], b.fq.at[x, e], to)
            b.fq[x, e] = b.tq[e, xl, X]

    def part4s(i):
        _, e, rel = place(i)

        @pl.when(rel == 0)
        def _():
            got("yr", (e, 0), b.yr.at[e])
            got("yr", (e, 1), b.yl.at[e])
            for Xd in (0, 1):
                b.us[e, Xd] = (
                    b.s[i, Xd].astype(F32) + b.yr[e, Xd].astype(F32) + b.yl[e, Xd].astype(F32)
                ).astype(BF16)
            send("fs", (e,), b.us.at[e, 1 - X], b.fs.at[X, e], dxo)
            b.fs[X, e] = b.us[e, X]

    def run(part, i, lag):
        pl.when((i >= lag) & (i < 8 + lag))(lambda: part(i - lag))

    ahead = 1 - lax.rem(c + X, 2)
    h_take(0)
    pl.when(ahead == 1)(lambda: h_take(1))
    part1(((0, 0), (0, 1)))
    pl.when(ahead == 0)(lambda: h_take(1))

    @pl.loop(0, 16)
    def _(n):
        @pl.when((n >= 2) & (n < 7))
        def _():
            h_take(n)

        run(part2s, n, 2)
        run(part2q, n, 2)
        for h in (0, 1):

            @pl.when((lax.rem(n, 2) == h) & (n < 6))
            def _():
                part1(((n - h + 1 + par, h), (n - h + 2 - par, 1 - h)))

        @pl.when(n == 6)
        def _():
            part1(((7, 0), (7, 1)))

        run(part4q, n, 5)
        run(part3s, n, 4)
        run(part4s, n, 8)

    def ph_last():
        for e in (0, 1):
            got("fq", (e,), b.fq.at[pl.ds(0, 3), e])
            got("fs", (e,), b.fs.at[0, e])
            for g in (0, 1):
                lanes = pl.ds(e * 256 + g * TB, TB)
                t = b.fq[2 * g, e].astype(F32) + b.fq[2 * g + 1, e].astype(F32)
                u = b.fs[g, e].astype(F32)
                primal = t[:KD]
                out[:, lanes] = primal.astype(BF16)
                sq = 1.0 / (1.0 + jnp.exp(-primal))
                slope = sq * (1.0 - sq)
                first, rest = NY - KD, 2 * KD - NY
                total = jnp.sum(slope[:first] * t[KD:] * t[KD:], axis=0, keepdims=True)
                total += jnp.sum(slope[first:] * u[:rest] * u[:rest], axis=0, keepdims=True)
                total += jnp.sum(slope * u[rest:] * u[rest:], axis=0, keepdims=True)
                b.cvs[:, lanes] = total

    ph_last()

    for r in range(1, 32):
        send("cv", (0,), b.cvs, b.cvr.at[r], peers[r - 1])
    got("cv", (0,), b.cvr.at[pl.ds(1, 31)])
    total = b.cvs[...]
    for r in range(1, 32):
        total += b.cvr[r]
    curv[...] = total / (PROBES * D)

    def ph_drain():
        for k in range(3):
            sent("tokx", tx, k)
        sent("toky", b.xg.at[pl.ds(0, 6)])
        sent("w1", b.w.at[pl.ds(0, KD), :])
        sent("m1", b.mx.at[0])
        sent("wr", b.w.at[pl.ds(0, 14 * KD), :])
        sent("wd", b.w.at[pl.ds(0, 16 * KD), :])

        @pl.when(c != X)
        def _():
            sent("hx", b.h.at[pl.ds(0, 2)])

        sent("hr", b.h.at[pl.ds(0, 14)])
        sent("hd", b.h.at[pl.ds(0, 16)])
        sent("px", b.rx)
        sent("qa", b.q.at[pl.ds(0, 2)])
        sent("qr", b.q.at[pl.ds(0, 4)])
        sent("ya", b.rx.at[pl.ds(0, 2)])
        sent("yr", b.rx.at[pl.ds(0, 4)])
        sent("fq", b.q.at[pl.ds(0, 3), 0])
        sent("fs", b.rx.at[0])
        sent("cv", b.cvr.at[pl.ds(1, 31)])

    ph_drain()


def on_device(tokens, norm_gain, gate_weight, up_weight, down_weight, probes):
    vmem = pl.BlockSpec(memory_space=pltpu.VMEM)
    hbm = pl.BlockSpec(memory_space=pl.ANY)
    sems = []
    for name, shape in SEMS.items():
        sems += [pltpu.SemaphoreType.DMA((3,) if name == "tokx" else (1,)), pltpu.SemaphoreType.DMA(shape)]
    out, curv = pl.pallas_call(
        kernel,
        out_shape=(pltpu.VMEM((KD, 512), BF16), pltpu.VMEM((1, 512), F32)),
        in_specs=[hbm] * 6,
        out_specs=(vmem, vmem),
        scratch_shapes=[pltpu.VMEM(s, t) for s, t in SCRATCH.values()] + sems + [pltpu.SemaphoreType.DMA((7,))],
        compiler_params=pltpu.CompilerParams(
            collective_id=0, has_side_effects=True, vmem_limit_bytes=60 * 1024 * 1024
        ),
        name="mlp_curv",
    )(tokens.T, norm_gain.reshape(28, 128), gate_weight, up_weight, down_weight, probes)
    return out.T, curv.reshape(512)


def solution(mesh):
    return jax.shard_map(
        on_device,
        mesh=mesh,
        in_specs=(
            P("fsdp", "tp"),
            P(),
            P("fsdp", "tp"),
            P("fsdp", "tp"),
            P("fsdp", "tp"),
            P(None, "fsdp", "tp"),
        ),
        out_specs=(P("tp", "fsdp"), P("tp")),
        check_vma=False,
    )
```

```python
import jax
import jax.numpy as jnp
from jax import lax
from jax.experimental import pallas as pl
from jax.experimental.pallas import tpu as pltpu
from jax.sharding import PartitionSpec as P

MESH = pl.DeviceIdType.MESH
F32, BF16 = jnp.float32, jnp.bfloat16
D = 3584
PROBES = 2
EPS = 1e-06
KD = 112
FH = 640
TB = 128
DT = 448
NY = 144
NX = 3 * KD - NY

SCRATCH = dict(
    tv=((DT, TB), BF16),
    gv=((28, 128), BF16),
    xg=((8, 256, DT), BF16),
    xn=((8, 256, DT), BF16),
    g8=((8, DT), F32),
    w=((D, 2 * FH), BF16),
    acc=((256, 2 * FH), F32),
    hs=((2, FH, TB), BF16),
    h=((32, FH, TB), BF16),
    mx=((2, 3 * KD, 2 * FH), BF16),
    px=((8, 2, NX, TB), BF16),
    rx=((8, 2, NX, TB), BF16),
    sx=((8, 2, NX, TB), F32),
    s=((8, 2, NX, TB), BF16),
    ya=((2, NX, TB), BF16),
    yb=((2, NX, TB), BF16),
    yr=((2, 2, NX, TB), BF16),
    yl=((2, 2, NX, TB), BF16),
    us=((2, 2, NX, TB), BF16),
    fs=((2, 2, NX, TB), BF16),
    q=((8, 2, 2, NY, TB), BF16),
    qa=((2, 2, NY, TB), BF16),
    qb=((2, 2, NY, TB), BF16),
    qr=((2, 2, 2, NY, TB), BF16),
    ql=((2, 2, 2, NY, TB), BF16),
    tq=((2, 2, 2, NY, TB), BF16),
    fq=((4, 2, NY, TB), BF16),
    cvs=((1, 512), F32),
    cvr=((32, 1, 512), F32),
)
SEMS = dict(
    tokx=(3,), toky=(2, 2, 2), w1=(1,), m1=(1,), wr=(2, 2, 4, 2), wd=(2, 8), hx=(2,), hr=(2, 4, 2), hd=(8, 2),
    px=(8,), qa=(2, 2), qr=(2, 2), ya=(2, 2), yr=(2, 2), fq=(2,), fs=(2,), cv=(1,),
)


class Refs:
    pass


def kernel(tok_t, gain, wg, wu, dn, pr, out, curv, *scratch):
    b, ss, rs = Refs(), Refs(), Refs()
    names = list(SCRATCH)
    for n, r in zip(names, scratch):
        setattr(b, n, r)
    rest = scratch[len(names):]
    for i, n in enumerate(SEMS):
        setattr(ss, n, rest[2 * i])
        setattr(rs, n, rest[2 * i + 1])
    loc = rest[2 * len(SEMS)]

    fi, ti = lax.axis_index("fsdp"), lax.axis_index("tp")
    X, z, c = fi // 16, lax.rem(fi // 2, 8), lax.rem(fi, 2)
    xl, y = ti // 4, lax.rem(ti, 4)
    x = X * 2 + xl

    def dev(x_=None, y_=None, z_=None, c_=None):
        x_ = x if x_ is None else x_
        y_ = y if y_ is None else y_
        z_ = z if z_ is None else z_
        c_ = c if c_ is None else c_
        return ((x_ // 2) * 16 + z_ * 2 + c_, lax.rem(x_, 2) * 4 + y_)

    xp, xm, xo = lax.rem(x + 1, 4), lax.rem(x + 3, 4), lax.rem(x + 2, 4)
    yp, ym = lax.rem(y + 1, 4), lax.rem(y + 3, 4)
    dxp, dxm, dxo = dev(x_=xp), dev(x_=xm), dev(x_=xo)
    dyp, dym = dev(y_=yp), dev(y_=ym)
    dz = (dev(z_=lax.rem(z + 1, 8)), dev(z_=lax.rem(z + 7, 8)))
    dc = dev(c_=1 - c)

    def copy(name, idx, src, dst, to):
        out_sem = getattr(ss, name).at[idx[0] if name == "tokx" else 0]
        return pltpu.make_async_remote_copy(
            src_ref=src, dst_ref=dst, send_sem=out_sem, recv_sem=getattr(rs, name).at[idx],
            device_id=to, device_id_type=MESH,
        )

    def send(name, idx, src, dst, to):
        copy(name, idx, src, dst, to).start()

    def got(name, idx, ref):
        copy(name, idx, ref, ref, dc).wait_recv()

    def sent(name, ref, idx=0):
        copy(name, (idx,) + (0,) * (len(SEMS[name]) - 1), ref, ref, dc).wait_send()

    def cols(k):
        return pl.ds(pl.multiple_of(k * FH, 128), FH)

    def wrows(X_, z_, c_=None):
        c_ = c if c_ is None else c_
        return pl.ds(pl.multiple_of((X_ * 16 + z_ * 2 + c_) * KD, 16), KD)

    def wchunk(X_, z_, half):
        return b.w.at[wrows(X_, z_), pl.ds(half * FH, FH)]

    def hchunk(X_, z_):
        return b.h.at[c * 16 + X_ * 8 + z_]

    mine = [
        (tok_t, b.tv),
        (gain, b.gv),
        (wg.at[:, cols(X)], wchunk(X, z, 0)),
        (wu.at[:, cols(X)], wchunk(X, z, 1)),
        (dn, b.mx.at[X, pl.ds(0, KD), :]),
        (pr.at[0], b.mx.at[X, pl.ds(KD, KD), :]),
        (pr.at[1], b.mx.at[X, pl.ds(2 * KD, KD), :]),
    ]
    own = [pltpu.make_async_copy(s_, d_, loc.at[i]) for i, (s_, d_) in enumerate(mine)]
    for o in own[2:4]:
        o.start()
    barrier = pltpu.get_barrier_semaphore()
    peers = [(lax.rem(fi + r, 32), ti) for r in range(1, 32)]
    partners = [dxp, dxm, dyp, dym] + peers
    for p in partners:
        pl.semaphore_signal(barrier, inc=1, device_id=p, device_id_type=MESH)
    for o in own[:2] + own[4:]:
        o.start()
    pl.semaphore_wait(barrier, len(partners))
    for o in own[2:4]:
        o.wait()

    def ring_start(sub, X_):
        for h in (0, 1):
            for d in (0, 1):
                ch = wchunk(X_, z, h ^ d)
                send("wr", (d, sub, 0, h ^ d), ch, ch, dz[d])
        send("wd", (sub, 0), b.w.at[wrows(X_, z), :], b.w.at[wrows(X_, z), :], dc)

    ring_start(0, X)
    tx = b.xg.at[ti, pl.ds(pl.multiple_of(X * TB, 128), TB), :]
    own[0].wait()
    tx[...] = b.tv[...].T
    for k, to in enumerate((dxp, dxm, dxo)):
        send("tokx", (k,), tx, tx, to)
    for half, src in enumerate((wg, wu)):
        send("w1", (0,), src.at[:, cols(1 - X)], wchunk(X, z, half), dxo)
    own[1].wait()
    for j in range(8):
        at = j * DT
        while at < (j + 1) * DT:
            n = min(128 - at % 128, (j + 1) * DT - at)
            row, lane = at // 128, at % 128
            b.g8[j : j + 1, at - j * DT : at - j * DT + n] = b.gv[row : row + 1, lane : lane + n].astype(F32)
            at += n
    for o in own[4:]:
        o.wait()

    def m_send():
        send("m1", (0,), b.mx.at[X], b.mx.at[X], dxo)

    def zsrc(d, s_):
        return lax.rem(z + (8 - s_ if d == 0 else s_), 8)

    def ring_half(sub, X_, s_, h):
        for d in (0, 1):
            ch = wchunk(X_, zsrc(d, s_), h ^ d)
            got("wr", (d, sub, s_ - 1, h ^ d), ch)
            if s_ < 3 or (s_ == 3 and h == 0):
                send("wr", (d, sub, s_, h ^ d), ch, ch, dz[d])
        if h == 1 or s_ == 4:
            for d in (0, 1):
                if s_ == 4 and d == 1:
                    continue
                blk = b.w.at[wrows(X_, zsrc(d, s_)), :]
                send("wd", (sub, 8 - s_ if d == 0 else s_), blk, blk, dc)

    par = lax.rem(z, 2)

    def pair(i):
        f = 3 * i - 5 * (i // 2) - 2 * (i // 3)
        return lax.rem(z // 2 + f * (1 - par) + (4 - f) * par, 4)

    def other_core(sub, X_, s_):
        if s_ == 1:
            got("wd", (sub, 0), b.w.at[wrows(X_, z, 1 - c), :])
        for d in (0, 1):
            if s_ == 4 and d == 1:
                continue
            got("wd", (sub, 8 - s_ if d == 0 else s_), b.w.at[wrows(X_, zsrc(d, s_), 1 - c), :])

    def multiply(X_, s_):
        j = X_ * 4 + pair(s_ - 1)

        @pl.loop(0, 5)
        def _(n):
            cs = pl.ds(pl.multiple_of(n * 256, 256), 256)
            ks = pl.ds(pl.multiple_of(j * DT, 64), DT)
            b.acc[:, cs] += jnp.dot(b.xn[j], b.w[ks, cs], preferred_element_type=F32)

    def tokx_done():
        for k, sx in enumerate((xm, xp, xo)):
            got("tokx", (k,), b.xg.at[lax.rem(sx, 2) * 4 + y, pl.ds(pl.multiple_of((sx // 2) * TB, 128), TB), :])
        for k in (0, 1):
            blk = b.xg.at[k * 4 + y]
            send("toky", (0, k, 0), blk, blk, dyp)
            send("toky", (1, k, 0), blk, blk, dym)

    def toky_first():
        for d, sy, to in ((0, ym, dyp), (1, yp, dym)):
            for k in (0, 1):
                got("toky", (d, k, 0), b.xg.at[k * 4 + sy])
            blk = b.xg.at[d * 4 + sy]
            send("toky", (d, d, 1), blk, blk, to)

    def toky_last():
        for d in (0, 1):
            got("toky", (d, d, 1), b.xg.at[d * 4 + lax.rem(y + 2, 4)])

    def norm():
        @pl.loop(0, 8)
        def _(t):
            rows = pl.ds(pl.multiple_of(t * 32, 32), 32)
            total = jnp.zeros((32, 1), F32)
            for j in range(8):
                v = b.xg[j, rows, :].astype(F32)
                total += jnp.sum(v * v, axis=1, keepdims=True)
            inv = lax.rsqrt(total / D + EPS)
            for j in range(8):
                v = b.xg[j, rows, :].astype(F32)
                b.xn[j, rows, :] = (v * inv * b.g8[j : j + 1, :]).astype(BF16)

    b.acc[...] = jnp.zeros_like(b.acc)
    ring_half(0, X, 1, 0)
    tokx_done()
    ring_half(0, X, 1, 1)
    ring_half(0, X, 2, 0)
    ring_half(0, X, 2, 1)
    ring_half(0, X, 3, 0)
    got("w1", (0,), b.w.at[wrows(1 - X, z), :])
    ring_start(1, 1 - X)
    ring_half(0, X, 3, 1)
    toky_first()
    m_send()
    ring_half(0, X, 4, 0)
    ring_half(1, 1 - X, 1, 0)
    ring_half(1, 1 - X, 1, 1)
    toky_last()
    norm()
    ready = {
        (2, 0): [(0, X, 1), (0, X, 2)],
        (2, 1): [(0, X, 3), (0, X, 4)],
        (3, 0): [(1, 1 - X, 1)],
        (3, 1): [(1, 1 - X, 2)],
    }
    for at, done in ready.items():
        ring_half(1, 1 - X, *at)
        for d in done:
            other_core(*d)
            multiply(*d[1:])
    ring_half(1, 1 - X, 4, 0)
    other_core(1, 1 - X, 3)
    multiply(1 - X, 3)
    other_core(1, 1 - X, 4)

    def swap(k, rows):
        src, dst = b.hs.at[k, rows], b.h.at[(1 - c) * 16 + k * 8 + z, rows]
        pl.when(c != X)(lambda: send("hx", (k,), src, dst, dev(x_=xo, c_=1 - c)))

    j = (1 - X) * 4 + pair(3)
    ks = pl.ds(pl.multiple_of(j * DT, 64), DT)
    for n in range(5):
        cs, us = pl.ds(n * 128, 128), pl.ds(FH + n * 128, 128)
        both = jnp.concatenate([b.w[ks, cs], b.w[ks, us]], axis=1)
        t = jnp.dot(b.xn[j], both, preferred_element_type=F32)
        g, u = b.acc[:, cs] + t[:, :128], b.acc[:, us] + t[:, 128:]
        hid = (g / (1.0 + jnp.exp(-g)) * u).T.astype(BF16)
        for k in (0, 1):
            part = hid[:, k * TB : (k + 1) * TB]
            b.hs[k, cs, :] = part

            @pl.when(c == X)
            def _():
                b.h[c * 16 + k * 8 + z, cs, :] = part

        if n:
            swap(0, pl.ds((n - 1) * 128, 128))
    swap(0, pl.ds(512, 128))
    swap(1, pl.ds(0, FH))

    got("m1", (0,), b.mx.at[1 - X])
    for k, ways in ((0, ((0, 0),)), (1, ((1, 1), (0, 1), (1, 0)))):

        @pl.when(c != X)
        def _():
            got("hx", (k,), hchunk(k, z))

        for d, kk in ways:
            send("hr", (d, 0, kk), hchunk(kk, z), hchunk(kk, z), dz[d])
        send("hd", (0, k), hchunk(k, z), hchunk(k, z), dc)

    def hother(k, z_):
        return b.h.at[(1 - c) * 16 + k * 8 + z_]

    def h_take(n):
        s_ = n // 2 + 1
        for h in (0, 1):

            @pl.when(lax.rem(n, 2) == h)
            def _():
                for d in (0, 1):
                    k = h ^ d
                    ch = hchunk(k, lax.rem(z + (8 - s_ if d == 0 else s_), 8))
                    got("hr", (d, s_ - 1, k), ch)

                    @pl.when(s_ < 4 - h)
                    def _():
                        send("hr", (d, s_, k), ch, ch, dz[d])

                    send("hd", (8 - s_ if d == 0 else s_, k), ch, ch, dc)

    def level(i):
        k = (i + 1) // 2
        r = lax.rem(i + par, 2) * (8 - 2 * k) + k
        return lax.rem(r, 8), lax.rem(z + r, 8)

    def place(i):
        _, zz = level(i)
        return zz, lax.rem(zz, 2), lax.rem(zz // 2 - y + 4, 4)

    def plus(u, v):
        return (u.astype(F32) + v.astype(F32)).astype(BF16)

    xn_ = (x // 2) * 2 + 1 - xl
    dxn = dev(x_=xn_)

    def part1(units):
        at = []
        for i, k in units:
            zz, e, rel = place(i)
            r, _ = level(i)
            got("hd", (r, k), hother(k, zz))
            at.append((k * 8 + zz, e, rel))
        halves = [jnp.concatenate([b.h[f * 16 + at[0][0]], b.h[f * 16 + at[1][0]]], axis=1) for f in (0, 1)]
        for Xd in (0, 1):
            t = jnp.dot(b.mx[Xd, :, :FH], halves[0], preferred_element_type=F32)
            t += jnp.dot(b.mx[Xd, :, FH:], halves[1], preferred_element_type=F32)
            for j, (i, k) in enumerate(units):
                u = t[:, j * TB : (j + 1) * TB]
                b.q[i, k, Xd] = u[:NY].astype(BF16)

                @pl.when(xl == k)
                def _():
                    b.sx[i, Xd] = u[NY:]

                @pl.when(xl != k)
                def _():
                    b.px[i, Xd] = u[NY:].astype(BF16)

            for (i, k), (_, e, rel) in zip(units, at):
                blk = b.q.at[i, k, Xd]

                @pl.when(xl != k)
                def _():
                    send("px", (i,), b.px.at[i, Xd], b.rx.at[i, Xd], dxn)

                @pl.when(rel == 2)
                def _():
                    send("qa", (e, k), blk, (b.qa if k == 0 else b.qb).at[e, Xd], dyp if k == 0 else dym)

                if k == 1:

                    @pl.when(rel == 1)
                    def _():
                        send("qr", (e, 0), blk, b.qr.at[e, 1, Xd], dyp)

                else:

                    @pl.when(rel == 3)
                    def _():
                        send("qr", (e, 1), blk, b.ql.at[e, 0, Xd], dym)

    def part2s(i):
        _, e, rel = place(i)
        got("px", (i,), b.rx.at[i])
        for Xd in (0, 1):
            b.s[i, Xd] = (b.sx[i, Xd] + b.rx[i, Xd].astype(F32)).astype(BF16)

        @pl.when(rel == 2)
        def _():
            send("ya", (e, 0), b.s.at[i, 0], b.ya.at[e], dyp)
            send("ya", (e, 1), b.s.at[i, 1], b.yb.at[e], dym)

        @pl.when(rel == 1)
        def _():
            send("yr", (e, 0), b.s.at[i, 1], b.yr.at[e, 1], dyp)

        @pl.when(rel == 3)
        def _():
            send("yr", (e, 1), b.s.at[i, 0], b.yl.at[e, 0], dym)

    def part2q(i):
        _, e, rel = place(i)

        @pl.when(rel == 1)
        def _():
            got("qa", (e, 0), b.qa.at[e])
            for Xd in (0, 1):
                b.q[i, 0, Xd] = plus(b.q[i, 0, Xd], b.qa[e, Xd])
            send("qr", (e, 0), b.q.at[i, 0], b.qr.at[e, 0], dyp)

        @pl.when(rel == 3)
        def _():
            got("qa", (e, 1), b.qb.at[e])
            for Xd in (0, 1):
                b.q[i, 1, Xd] = plus(b.q[i, 1, Xd], b.qb[e, Xd])
            send("qr", (e, 1), b.q.at[i, 1], b.ql.at[e, 1], dym)

    def part3s(i):
        _, e, rel = place(i)

        @pl.when(rel == 1)
        def _():
            got("ya", (e, 0), b.ya.at[e])
            b.s[i, 0] = plus(b.s[i, 0], b.ya[e])
            send("yr", (e, 0), b.s.at[i, 0], b.yr.at[e, 0], dyp)

        @pl.when(rel == 3)
        def _():
            got("ya", (e, 1), b.yb.at[e])
            b.s[i, 1] = plus(b.s[i, 1], b.yb[e])
            send("yr", (e, 1), b.s.at[i, 1], b.yl.at[e, 1], dym)

    def part4q(i):
        _, e, rel = place(i)

        @pl.when(rel == 0)
        def _():
            got("qr", (e, 0), b.qr.at[e])
            got("qr", (e, 1), b.ql.at[e])

            @pl.loop(0, 4)
            def _(dx):
                at = (lax.rem(dx, 2), dx // 2)
                u = b.q[i, *at].astype(F32) + b.qr[e, *at].astype(F32) + b.ql[e, *at].astype(F32)
                b.tq[e, *at] = u.astype(BF16)

            for to, tx_ in ((dxo, xo), (dxp, xp), (dxm, xm)):
                send("fq", (e,), b.tq.at[e, lax.rem(tx_, 2), tx_ // 2], b.fq.at[x, e], to)
            b.fq[x, e] = b.tq[e, xl, X]

    def part4s(i):
        _, e, rel = place(i)

        @pl.when(rel == 0)
        def _():
            got("yr", (e, 0), b.yr.at[e])
            got("yr", (e, 1), b.yl.at[e])
            for Xd in (0, 1):
                b.us[e, Xd] = (
                    b.s[i, Xd].astype(F32) + b.yr[e, Xd].astype(F32) + b.yl[e, Xd].astype(F32)
                ).astype(BF16)
            send("fs", (e,), b.us.at[e, 1 - X], b.fs.at[X, e], dxo)
            b.fs[X, e] = b.us[e, X]

    def run(part, i, lag):
        pl.when((i >= lag) & (i < 8 + lag))(lambda: part(i - lag))

    ahead = 1 - lax.rem(c + X, 2)
    h_take(0)
    pl.when(ahead == 1)(lambda: h_take(1))
    part1(((0, 0), (0, 1)))
    pl.when(ahead == 0)(lambda: h_take(1))

    @pl.loop(0, 16)
    def _(n):
        @pl.when((n >= 2) & (n < 7))
        def _():
            h_take(n)

        run(part2s, n, 2)
        run(part2q, n, 2)
        for h in (0, 1):

            @pl.when((lax.rem(n, 2) == h) & (n < 6))
            def _():
                part1(((n - h + 1 + par, h), (n - h + 2 - par, 1 - h)))

        @pl.when(n == 6)
        def _():
            part1(((7, 0), (7, 1)))

        run(part4q, n, 5)
        run(part3s, n, 4)
        run(part4s, n, 8)

    def ph_last():
        for e in (0, 1):
            got("fq", (e,), b.fq.at[pl.ds(0, 3), e])
            got("fs", (e,), b.fs.at[0, e])
            for g in (0, 1):
                lanes = pl.ds(e * 256 + g * TB, TB)
                t = b.fq[2 * g, e].astype(F32) + b.fq[2 * g + 1, e].astype(F32)
                u = b.fs[g, e].astype(F32)
                primal = t[:KD]
                out[:, lanes] = primal.astype(BF16)
                sq = 1.0 / (1.0 + jnp.exp(-primal))
                slope = sq * (1.0 - sq)
                first, rest = NY - KD, 2 * KD - NY
                total = jnp.sum(slope[:first] * t[KD:] * t[KD:], axis=0, keepdims=True)
                total += jnp.sum(slope[first:] * u[:rest] * u[:rest], axis=0, keepdims=True)
                total += jnp.sum(slope * u[rest:] * u[rest:], axis=0, keepdims=True)
                b.cvs[:, lanes] = total

    ph_last()

    for r in sorted(range(1, 32), key=lambda r: -min(r // 2 % 8, 8 - r // 2 % 8)):
        send("cv", (0,), b.cvs, b.cvr.at[r], peers[r - 1])
    got("cv", (0,), b.cvr.at[pl.ds(1, 31)])
    total = b.cvs[...]
    for r in range(1, 32):
        total += b.cvr[r]
    curv[...] = total / (PROBES * D)

    def ph_drain():
        for k in range(3):
            sent("tokx", tx, k)
        sent("toky", b.xg.at[pl.ds(0, 6)])
        sent("w1", b.w.at[pl.ds(0, KD), :])
        sent("m1", b.mx.at[0])
        sent("wr", b.w.at[pl.ds(0, 14 * KD), :])
        sent("wd", b.w.at[pl.ds(0, 16 * KD), :])

        @pl.when(c != X)
        def _():
            sent("hx", b.h.at[pl.ds(0, 2)])

        sent("hr", b.h.at[pl.ds(0, 14)])
        sent("hd", b.h.at[pl.ds(0, 16)])
        sent("px", b.rx)
        sent("qa", b.q.at[pl.ds(0, 2)])
        sent("qr", b.q.at[pl.ds(0, 4)])
        sent("ya", b.rx.at[pl.ds(0, 2)])
        sent("yr", b.rx.at[pl.ds(0, 4)])
        sent("fq", b.q.at[pl.ds(0, 3), 0])
        sent("fs", b.rx.at[0])
        sent("cv", b.cvr.at[pl.ds(1, 31)])

    ph_drain()


def on_device(tokens, norm_gain, gate_weight, up_weight, down_weight, probes):
    vmem = pl.BlockSpec(memory_space=pltpu.VMEM)
    hbm = pl.BlockSpec(memory_space=pl.ANY)
    sems = []
    for name, shape in SEMS.items():
        sems += [pltpu.SemaphoreType.DMA((3,) if name == "tokx" else (1,)), pltpu.SemaphoreType.DMA(shape)]
    out, curv = pl.pallas_call(
        kernel,
        out_shape=(pltpu.VMEM((KD, 512), BF16), pltpu.VMEM((1, 512), F32)),
        in_specs=[hbm] * 6,
        out_specs=(vmem, vmem),
        scratch_shapes=[pltpu.VMEM(s, t) for s, t in SCRATCH.values()] + sems + [pltpu.SemaphoreType.DMA((7,))],
        compiler_params=pltpu.CompilerParams(
            collective_id=0, has_side_effects=True, vmem_limit_bytes=60 * 1024 * 1024
        ),
        name="mlp_curv",
    )(tokens.T, norm_gain.reshape(28, 128), gate_weight, up_weight, down_weight, probes)
    return out.T, curv.reshape(512)


def solution(mesh):
    return jax.shard_map(
        on_device,
        mesh=mesh,
        in_specs=(
            P("fsdp", "tp"),
            P(),
            P("fsdp", "tp"),
            P("fsdp", "tp"),
            P("fsdp", "tp"),
            P(None, "fsdp", "tp"),
        ),
        out_specs=(P("tp", "fsdp"), P("tp")),
        check_vma=False,
    )
```

```python
import jax
import jax.numpy as jnp
from jax import lax
from jax.experimental import pallas as pl
from jax.experimental.pallas import tpu as pltpu
from jax.sharding import PartitionSpec as P

MESH = pl.DeviceIdType.MESH
F32, BF16 = jnp.float32, jnp.bfloat16
D = 3584
PROBES = 2
EPS = 1e-06
KD = 112
FH = 640
TB = 128
DT = 448
NY = 176
NX = 3 * KD - NY

SCRATCH = dict(
    tv=((DT, TB), BF16),
    gv=((28, 128), BF16),
    xg=((8, 256, DT), BF16),
    xn=((8, 256, DT), BF16),
    g8=((8, DT), F32),
    w=((D, 2 * FH), BF16),
    acc=((256, 2 * FH), F32),
    hs=((2, FH, TB), BF16),
    h=((32, FH, TB), BF16),
    mx=((2, 3 * KD, 2 * FH), BF16),
    px=((8, 2, NX, TB), BF16),
    rx=((8, 2, NX, TB), BF16),
    sx=((8, 2, NX, TB), F32),
    s=((8, 2, NX, TB), BF16),
    ya=((2, NX, TB), BF16),
    yb=((2, NX, TB), BF16),
    yr=((2, 2, NX, TB), BF16),
    yl=((2, 2, NX, TB), BF16),
    us=((2, 2, NX, TB), BF16),
    fs=((2, 2, NX, TB), BF16),
    q=((8, 2, 2, NY, TB), BF16),
    qa=((2, 2, NY, TB), BF16),
    qb=((2, 2, NY, TB), BF16),
    qr=((2, 2, 2, NY, TB), BF16),
    ql=((2, 2, 2, NY, TB), BF16),
    tq=((2, 2, 2, NY, TB), BF16),
    fq=((4, 2, NY, TB), BF16),
    cvs=((1, 512), F32),
    cvr=((32, 1, 512), F32),
)
SEMS = dict(
    tokx=(3,), toky=(2, 2, 2), w1=(1,), m1=(1,), wr=(2, 2, 4, 2), wd=(2, 8), hx=(2,), hr=(2, 4, 2), hd=(8, 2),
    px=(8,), qa=(2, 2), qr=(2, 2), ya=(2, 2), yr=(2, 2), fq=(2,), fs=(2,), cv=(1,),
)


class Refs:
    pass


def kernel(tok_t, gain, wg, wu, dn, pr, out, curv, *scratch):
    b, ss, rs = Refs(), Refs(), Refs()
    names = list(SCRATCH)
    for n, r in zip(names, scratch):
        setattr(b, n, r)
    rest = scratch[len(names):]
    for i, n in enumerate(SEMS):
        setattr(ss, n, rest[2 * i])
        setattr(rs, n, rest[2 * i + 1])
    loc = rest[2 * len(SEMS)]

    fi, ti = lax.axis_index("fsdp"), lax.axis_index("tp")
    X, z, c = fi // 16, lax.rem(fi // 2, 8), lax.rem(fi, 2)
    xl, y = ti // 4, lax.rem(ti, 4)
    x = X * 2 + xl

    def dev(x_=None, y_=None, z_=None, c_=None):
        x_ = x if x_ is None else x_
        y_ = y if y_ is None else y_
        z_ = z if z_ is None else z_
        c_ = c if c_ is None else c_
        return ((x_ // 2) * 16 + z_ * 2 + c_, lax.rem(x_, 2) * 4 + y_)

    xp, xm, xo = lax.rem(x + 1, 4), lax.rem(x + 3, 4), lax.rem(x + 2, 4)
    yp, ym = lax.rem(y + 1, 4), lax.rem(y + 3, 4)
    dxp, dxm, dxo = dev(x_=xp), dev(x_=xm), dev(x_=xo)
    dyp, dym = dev(y_=yp), dev(y_=ym)
    dz = (dev(z_=lax.rem(z + 1, 8)), dev(z_=lax.rem(z + 7, 8)))
    dc = dev(c_=1 - c)

    def copy(name, idx, src, dst, to):
        out_sem = getattr(ss, name).at[idx[0] if name == "tokx" else 0]
        return pltpu.make_async_remote_copy(
            src_ref=src, dst_ref=dst, send_sem=out_sem, recv_sem=getattr(rs, name).at[idx],
            device_id=to, device_id_type=MESH,
        )

    def send(name, idx, src, dst, to):
        copy(name, idx, src, dst, to).start()

    def got(name, idx, ref):
        copy(name, idx, ref, ref, dc).wait_recv()

    def sent(name, ref, idx=0):
        copy(name, (idx,) + (0,) * (len(SEMS[name]) - 1), ref, ref, dc).wait_send()

    def cols(k):
        return pl.ds(pl.multiple_of(k * FH, 128), FH)

    def wrows(X_, z_, c_=None):
        c_ = c if c_ is None else c_
        return pl.ds(pl.multiple_of((X_ * 16 + z_ * 2 + c_) * KD, 16), KD)

    def wchunk(X_, z_, half):
        return b.w.at[wrows(X_, z_), pl.ds(half * FH, FH)]

    def hchunk(X_, z_):
        return b.h.at[c * 16 + X_ * 8 + z_]

    mine = [
        (tok_t, b.tv),
        (gain, b.gv),
        (wg.at[:, cols(X)], wchunk(X, z, 0)),
        (wu.at[:, cols(X)], wchunk(X, z, 1)),
        (dn, b.mx.at[X, pl.ds(0, KD), :]),
        (pr.at[0], b.mx.at[X, pl.ds(KD, KD), :]),
        (pr.at[1], b.mx.at[X, pl.ds(2 * KD, KD), :]),
    ]
    own = [pltpu.make_async_copy(s_, d_, loc.at[i]) for i, (s_, d_) in enumerate(mine)]
    for o in own[2:4]:
        o.start()
    barrier = pltpu.get_barrier_semaphore()
    peers = [(lax.rem(fi + r, 32), ti) for r in range(1, 32)]
    partners = [dxp, dxm, dyp, dym] + peers
    for p in partners:
        pl.semaphore_signal(barrier, inc=1, device_id=p, device_id_type=MESH)
    for o in own[:2] + own[4:]:
        o.start()
    pl.semaphore_wait(barrier, len(partners))
    for o in own[2:4]:
        o.wait()

    def ring_start(sub, X_):
        for h in (0, 1):
            for d in (0, 1):
                ch = wchunk(X_, z, h ^ d)
                send("wr", (d, sub, 0, h ^ d), ch, ch, dz[d])
        send("wd", (sub, 0), b.w.at[wrows(X_, z), :], b.w.at[wrows(X_, z), :], dc)

    ring_start(0, X)
    tx = b.xg.at[ti, pl.ds(pl.multiple_of(X * TB, 128), TB), :]
    own[0].wait()
    tx[...] = b.tv[...].T
    for k, to in enumerate((dxp, dxm, dxo)):
        send("tokx", (k,), tx, tx, to)
    for half, src in enumerate((wg, wu)):
        send("w1", (0,), src.at[:, cols(1 - X)], wchunk(X, z, half), dxo)
    own[1].wait()
    for j in range(8):
        at = j * DT
        while at < (j + 1) * DT:
            n = min(128 - at % 128, (j + 1) * DT - at)
            row, lane = at // 128, at % 128
            b.g8[j : j + 1, at - j * DT : at - j * DT + n] = b.gv[row : row + 1, lane : lane + n].astype(F32)
            at += n
    for o in own[4:]:
        o.wait()

    def m_send():
        send("m1", (0,), b.mx.at[X], b.mx.at[X], dxo)

    def zsrc(d, s_):
        return lax.rem(z + (8 - s_ if d == 0 else s_), 8)

    def ring_half(sub, X_, s_, h):
        for d in (0, 1):
            ch = wchunk(X_, zsrc(d, s_), h ^ d)
            got("wr", (d, sub, s_ - 1, h ^ d), ch)
            if s_ < 3 or (s_ == 3 and h == 0):
                send("wr", (d, sub, s_, h ^ d), ch, ch, dz[d])
        if h == 1 or s_ == 4:
            for d in (0, 1):
                if s_ == 4 and d == 1:
                    continue
                blk = b.w.at[wrows(X_, zsrc(d, s_)), :]
                send("wd", (sub, 8 - s_ if d == 0 else s_), blk, blk, dc)

    par = lax.rem(z, 2)

    def pair(i):
        f = 3 * i - 5 * (i // 2) - 2 * (i // 3)
        return lax.rem(z // 2 + f * (1 - par) + (4 - f) * par, 4)

    def other_core(sub, X_, s_):
        if s_ == 1:
            got("wd", (sub, 0), b.w.at[wrows(X_, z, 1 - c), :])
        for d in (0, 1):
            if s_ == 4 and d == 1:
                continue
            got("wd", (sub, 8 - s_ if d == 0 else s_), b.w.at[wrows(X_, zsrc(d, s_), 1 - c), :])

    def multiply(X_, s_):
        j = X_ * 4 + pair(s_ - 1)

        @pl.loop(0, 5)
        def _(n):
            cs = pl.ds(pl.multiple_of(n * 256, 256), 256)
            ks = pl.ds(pl.multiple_of(j * DT, 64), DT)
            b.acc[:, cs] += jnp.dot(b.xn[j], b.w[ks, cs], preferred_element_type=F32)

    def tokx_done():
        for k, sx in enumerate((xm, xp, xo)):
            got("tokx", (k,), b.xg.at[lax.rem(sx, 2) * 4 + y, pl.ds(pl.multiple_of((sx // 2) * TB, 128), TB), :])
        for k in (0, 1):
            blk = b.xg.at[k * 4 + y]
            send("toky", (0, k, 0), blk, blk, dyp)
            send("toky", (1, k, 0), blk, blk, dym)

    def toky_first():
        for d, sy, to in ((0, ym, dyp), (1, yp, dym)):
            for k in (0, 1):
                got("toky", (d, k, 0), b.xg.at[k * 4 + sy])
            blk = b.xg.at[d * 4 + sy]
            send("toky", (d, d, 1), blk, blk, to)

    def toky_last():
        for d in (0, 1):
            got("toky", (d, d, 1), b.xg.at[d * 4 + lax.rem(y + 2, 4)])

    def norm():
        @pl.loop(0, 8)
        def _(t):
            rows = pl.ds(pl.multiple_of(t * 32, 32), 32)
            total = jnp.zeros((32, 1), F32)
            for j in range(8):
                v = b.xg[j, rows, :].astype(F32)
                total += jnp.sum(v * v, axis=1, keepdims=True)
            inv = lax.rsqrt(total / D + EPS)
            for j in range(8):
                v = b.xg[j, rows, :].astype(F32)
                b.xn[j, rows, :] = (v * inv * b.g8[j : j + 1, :]).astype(BF16)

    b.acc[...] = jnp.zeros_like(b.acc)
    ring_half(0, X, 1, 0)
    tokx_done()
    ring_half(0, X, 1, 1)
    ring_half(0, X, 2, 0)
    ring_half(0, X, 2, 1)
    ring_half(0, X, 3, 0)
    got("w1", (0,), b.w.at[wrows(1 - X, z), :])
    ring_start(1, 1 - X)
    ring_half(0, X, 3, 1)
    toky_first()
    m_send()
    ring_half(0, X, 4, 0)
    ring_half(1, 1 - X, 1, 0)
    ring_half(1, 1 - X, 1, 1)
    toky_last()
    norm()
    ready = {
        (2, 0): [(0, X, 1), (0, X, 2)],
        (2, 1): [(0, X, 3), (0, X, 4)],
        (3, 0): [(1, 1 - X, 1)],
        (3, 1): [(1, 1 - X, 2)],
    }
    for at, done in ready.items():
        ring_half(1, 1 - X, *at)
        for d in done:
            other_core(*d)
            multiply(*d[1:])
    ring_half(1, 1 - X, 4, 0)
    other_core(1, 1 - X, 3)
    multiply(1 - X, 3)
    other_core(1, 1 - X, 4)

    def swap(k, rows):
        src, dst = b.hs.at[k, rows], b.h.at[(1 - c) * 16 + k * 8 + z, rows]
        pl.when(c != X)(lambda: send("hx", (k,), src, dst, dev(x_=xo, c_=1 - c)))

    j = (1 - X) * 4 + pair(3)
    ks = pl.ds(pl.multiple_of(j * DT, 64), DT)
    for n in range(5):
        cs, us = pl.ds(n * 128, 128), pl.ds(FH + n * 128, 128)
        both = jnp.concatenate([b.w[ks, cs], b.w[ks, us]], axis=1)
        t = jnp.dot(b.xn[j], both, preferred_element_type=F32)
        g, u = b.acc[:, cs] + t[:, :128], b.acc[:, us] + t[:, 128:]
        hid = (g / (1.0 + jnp.exp(-g)) * u).T.astype(BF16)
        for k in (0, 1):
            part = hid[:, k * TB : (k + 1) * TB]
            b.hs[k, cs, :] = part

            @pl.when(c == X)
            def _():
                b.h[c * 16 + k * 8 + z, cs, :] = part

        if n:
            swap(0, pl.ds((n - 1) * 128, 128))
    swap(0, pl.ds(512, 128))
    swap(1, pl.ds(0, FH))

    got("m1", (0,), b.mx.at[1 - X])
    for k, ways in ((0, ((0, 0),)), (1, ((1, 1), (0, 1), (1, 0)))):

        @pl.when(c != X)
        def _():
            got("hx", (k,), hchunk(k, z))

        for d, kk in ways:
            send("hr", (d, 0, kk), hchunk(kk, z), hchunk(kk, z), dz[d])
        send("hd", (0, k), hchunk(k, z), hchunk(k, z), dc)

    def hother(k, z_):
        return b.h.at[(1 - c) * 16 + k * 8 + z_]

    def h_take(n):
        s_ = n // 2 + 1
        for h in (0, 1):

            @pl.when(lax.rem(n, 2) == h)
            def _():
                for d in (0, 1):
                    k = h ^ d
                    ch = hchunk(k, lax.rem(z + (8 - s_ if d == 0 else s_), 8))
                    got("hr", (d, s_ - 1, k), ch)

                    @pl.when(s_ < 4 - h)
                    def _():
                        send("hr", (d, s_, k), ch, ch, dz[d])

                    send("hd", (8 - s_ if d == 0 else s_, k), ch, ch, dc)

    def level(i):
        k = (i + 1) // 2
        r = lax.rem(i + par, 2) * (8 - 2 * k) + k
        return lax.rem(r, 8), lax.rem(z + r, 8)

    def place(i):
        _, zz = level(i)
        return zz, lax.rem(zz, 2), lax.rem(zz // 2 - y + 4, 4)

    def plus(u, v):
        return (u.astype(F32) + v.astype(F32)).astype(BF16)

    xn_ = (x // 2) * 2 + 1 - xl
    dxn = dev(x_=xn_)

    def part1(units):
        at = []
        for i, k in units:
            zz, e, rel = place(i)
            r, _ = level(i)
            got("hd", (r, k), hother(k, zz))
            at.append((k * 8 + zz, e, rel))
        halves = [jnp.concatenate([b.h[f * 16 + at[0][0]], b.h[f * 16 + at[1][0]]], axis=1) for f in (0, 1)]
        for Xd in (0, 1):
            t = jnp.dot(b.mx[Xd, :, :FH], halves[0], preferred_element_type=F32)
            t += jnp.dot(b.mx[Xd, :, FH:], halves[1], preferred_element_type=F32)
            for j, (i, k) in enumerate(units):
                u = t[:, j * TB : (j + 1) * TB]
                b.q[i, k, Xd] = u[:NY].astype(BF16)

                @pl.when(xl == k)
                def _():
                    b.sx[i, Xd] = u[NY:]

                @pl.when(xl != k)
                def _():
                    b.px[i, Xd] = u[NY:].astype(BF16)

            for (i, k), (_, e, rel) in zip(units, at):
                blk = b.q.at[i, k, Xd]

                @pl.when(xl != k)
                def _():
                    send("px", (i,), b.px.at[i, Xd], b.rx.at[i, Xd], dxn)

                @pl.when(rel == 2)
                def _():
                    send("qa", (e, k), blk, (b.qa if k == 0 else b.qb).at[e, Xd], dyp if k == 0 else dym)

                if k == 1:

                    @pl.when(rel == 1)
                    def _():
                        send("qr", (e, 0), blk, b.qr.at[e, 1, Xd], dyp)

                else:

                    @pl.when(rel == 3)
                    def _():
                        send("qr", (e, 1), blk, b.ql.at[e, 0, Xd], dym)

    def part2s(i):
        _, e, rel = place(i)
        got("px", (i,), b.rx.at[i])
        for Xd in (0, 1):
            b.s[i, Xd] = (b.sx[i, Xd] + b.rx[i, Xd].astype(F32)).astype(BF16)

        @pl.when(rel == 2)
        def _():
            send("ya", (e, 0), b.s.at[i, 0], b.ya.at[e], dyp)
            send("ya", (e, 1), b.s.at[i, 1], b.yb.at[e], dym)

        @pl.when(rel == 1)
        def _():
            send("yr", (e, 0), b.s.at[i, 1], b.yr.at[e, 1], dyp)

        @pl.when(rel == 3)
        def _():
            send("yr", (e, 1), b.s.at[i, 0], b.yl.at[e, 0], dym)

    def part2q(i):
        _, e, rel = place(i)

        @pl.when(rel == 1)
        def _():
            got("qa", (e, 0), b.qa.at[e])
            for Xd in (0, 1):
                b.q[i, 0, Xd] = plus(b.q[i, 0, Xd], b.qa[e, Xd])
            send("qr", (e, 0), b.q.at[i, 0], b.qr.at[e, 0], dyp)

        @pl.when(rel == 3)
        def _():
            got("qa", (e, 1), b.qb.at[e])
            for Xd in (0, 1):
                b.q[i, 1, Xd] = plus(b.q[i, 1, Xd], b.qb[e, Xd])
            send("qr", (e, 1), b.q.at[i, 1], b.ql.at[e, 1], dym)

    def part3s(i):
        _, e, rel = place(i)

        @pl.when(rel == 1)
        def _():
            got("ya", (e, 0), b.ya.at[e])
            b.s[i, 0] = plus(b.s[i, 0], b.ya[e])
            send("yr", (e, 0), b.s.at[i, 0], b.yr.at[e, 0], dyp)

        @pl.when(rel == 3)
        def _():
            got("ya", (e, 1), b.yb.at[e])
            b.s[i, 1] = plus(b.s[i, 1], b.yb[e])
            send("yr", (e, 1), b.s.at[i, 1], b.yl.at[e, 1], dym)

    def part4q(i):
        _, e, rel = place(i)

        @pl.when(rel == 0)
        def _():
            got("qr", (e, 0), b.qr.at[e])
            got("qr", (e, 1), b.ql.at[e])

            @pl.loop(0, 4)
            def _(dx):
                at = (lax.rem(dx, 2), dx // 2)
                u = b.q[i, *at].astype(F32) + b.qr[e, *at].astype(F32) + b.ql[e, *at].astype(F32)
                b.tq[e, *at] = u.astype(BF16)

            for to, tx_ in ((dxo, xo), (dxp, xp), (dxm, xm)):
                send("fq", (e,), b.tq.at[e, lax.rem(tx_, 2), tx_ // 2], b.fq.at[x, e], to)
            b.fq[x, e] = b.tq[e, xl, X]

    def part4s(i):
        _, e, rel = place(i)

        @pl.when(rel == 0)
        def _():
            got("yr", (e, 0), b.yr.at[e])
            got("yr", (e, 1), b.yl.at[e])
            for Xd in (0, 1):
                b.us[e, Xd] = (
                    b.s[i, Xd].astype(F32) + b.yr[e, Xd].astype(F32) + b.yl[e, Xd].astype(F32)
                ).astype(BF16)
            send("fs", (e,), b.us.at[e, 1 - X], b.fs.at[X, e], dxo)
            b.fs[X, e] = b.us[e, X]

    def run(part, i, lag):
        pl.when((i >= lag) & (i < 8 + lag))(lambda: part(i - lag))

    ahead = 1 - lax.rem(c + X, 2)
    h_take(0)
    pl.when(ahead == 1)(lambda: h_take(1))
    part1(((0, 0), (0, 1)))
    pl.when(ahead == 0)(lambda: h_take(1))

    @pl.loop(0, 16)
    def _(n):
        @pl.when((n >= 2) & (n < 7))
        def _():
            h_take(n)

        run(part2s, n, 2)
        run(part2q, n, 2)
        for h in (0, 1):

            @pl.when((lax.rem(n, 2) == h) & (n < 6))
            def _():
                part1(((n - h + 1 + par, h), (n - h + 2 - par, 1 - h)))

        @pl.when(n == 6)
        def _():
            part1(((7, 0), (7, 1)))

        run(part4q, n, 5)
        run(part3s, n, 4)
        run(part4s, n, 8)

    def ph_last():
        for e in (0, 1):
            got("fq", (e,), b.fq.at[pl.ds(0, 3), e])
            got("fs", (e,), b.fs.at[0, e])
            for g in (0, 1):
                lanes = pl.ds(e * 256 + g * TB, TB)
                t = b.fq[2 * g, e].astype(F32) + b.fq[2 * g + 1, e].astype(F32)
                u = b.fs[g, e].astype(F32)
                primal = t[:KD]
                out[:, lanes] = primal.astype(BF16)
                sq = 1.0 / (1.0 + jnp.exp(-primal))
                slope = sq * (1.0 - sq)
                first, rest = NY - KD, 2 * KD - NY
                total = jnp.sum(slope[:first] * t[KD:] * t[KD:], axis=0, keepdims=True)
                total += jnp.sum(slope[first:] * u[:rest] * u[:rest], axis=0, keepdims=True)
                total += jnp.sum(slope * u[rest:] * u[rest:], axis=0, keepdims=True)
                b.cvs[:, lanes] = total

    ph_last()

    for r in sorted(range(1, 32), key=lambda r: -min(r // 2 % 8, 8 - r // 2 % 8)):
        send("cv", (0,), b.cvs, b.cvr.at[r], peers[r - 1])
    got("cv", (0,), b.cvr.at[pl.ds(1, 31)])
    total = b.cvs[...]
    for r in range(1, 32):
        total += b.cvr[r]
    curv[...] = total / (PROBES * D)

    def ph_drain():
        for k in range(3):
            sent("tokx", tx, k)
        sent("toky", b.xg.at[pl.ds(0, 6)])
        sent("w1", b.w.at[pl.ds(0, KD), :])
        sent("m1", b.mx.at[0])
        sent("wr", b.w.at[pl.ds(0, 14 * KD), :])
        sent("wd", b.w.at[pl.ds(0, 16 * KD), :])

        @pl.when(c != X)
        def _():
            sent("hx", b.h.at[pl.ds(0, 2)])

        sent("hr", b.h.at[pl.ds(0, 14)])
        sent("hd", b.h.at[pl.ds(0, 16)])
        sent("px", b.rx)
        sent("qa", b.q.at[pl.ds(0, 2)])
        sent("qr", b.q.at[pl.ds(0, 4)])
        sent("ya", b.rx.at[pl.ds(0, 2)])
        sent("yr", b.rx.at[pl.ds(0, 4)])
        sent("fq", b.q.at[pl.ds(0, 3), 0])
        sent("fs", b.rx.at[0])
        sent("cv", b.cvr.at[pl.ds(1, 31)])

    ph_drain()


def on_device(tokens, norm_gain, gate_weight, up_weight, down_weight, probes):
    vmem = pl.BlockSpec(memory_space=pltpu.VMEM)
    hbm = pl.BlockSpec(memory_space=pl.ANY)
    sems = []
    for name, shape in SEMS.items():
        sems += [pltpu.SemaphoreType.DMA((3,) if name == "tokx" else (1,)), pltpu.SemaphoreType.DMA(shape)]
    out, curv = pl.pallas_call(
        kernel,
        out_shape=(pltpu.VMEM((KD, 512), BF16), pltpu.VMEM((1, 512), F32)),
        in_specs=[hbm] * 6,
        out_specs=(vmem, vmem),
        scratch_shapes=[pltpu.VMEM(s, t) for s, t in SCRATCH.values()] + sems + [pltpu.SemaphoreType.DMA((7,))],
        compiler_params=pltpu.CompilerParams(
            collective_id=0, has_side_effects=True, vmem_limit_bytes=60 * 1024 * 1024
        ),
        name="mlp_curv",
    )(tokens.T, norm_gain.reshape(28, 128), gate_weight, up_weight, down_weight, probes)
    return out.T, curv.reshape(512)


def solution(mesh):
    return jax.shard_map(
        on_device,
        mesh=mesh,
        in_specs=(
            P("fsdp", "tp"),
            P(),
            P("fsdp", "tp"),
            P("fsdp", "tp"),
            P("fsdp", "tp"),
            P(None, "fsdp", "tp"),
        ),
        out_specs=(P("tp", "fsdp"), P("tp")),
        check_vma=False,
    )
```
